32 devices in a mesh: batch: 8 (over z, y), mp: 4 (over x, core).
Axes of the slice: x: 2, y: 2, z: 4, core: 2. Of those that a mesh axis runs over, the one named last changes fastest.
Arguments:
- init_state: float32 [4096, 256], P(('batch', 'mp')), may hold values from -6 to 6
- brownian: bfloat16 [32, 4096, 256], P(None, ('batch', 'mp')), may hold values from -6 to 6
- step_size: float32 [4096], P(('batch', 'mp')), may hold values from 0.02 to 0.1
- lengths: int32 [4096], P(('batch', 'mp')), may hold values from 1 to 32, as said below
- obs_steps: int32 [4096, 8], P(('batch', 'mp')), may hold values from 1 to 32, as said below
- observed: bfloat16 [4096, 8, 128], P(('batch', 'mp')), may hold values from -6 to 6
- w_in: bfloat16 [256, 1024], P(None, 'mp'), may hold values from -0.375 to 0.375
- b_in: bfloat16 [1024], P('mp'), may hold values from -3 to 3
- w_out: bfloat16 [1024, 256], P('mp'), may hold values from -0.1875 to 0.1875
- b_out: float32 [256], replicated, may hold values from -4 to 4
- decoder: bfloat16 [256, 128], replicated, may hold values from -0.375 to 0.375
- prior_rate: float32 [256], replicated, may hold values from 0.1 to 2
- diffusion: float32 [256], replicated, may hold values from 0.7 to 1.4
Outputs:
- elbo_series: float32 [4096], P(('batch', 'mp'))
- scores: float32 [2], replicated
- grad_w_in: float32 [256, 1024], P(None, 'mp')
- grad_b_in: float32 [1024], P('mp')
- grad_w_out: float32 [1024, 256], P('mp')
- grad_b_out: float32 [256], replicated
- grad_decoder: float32 [256, 128], replicated
- grad_init: float32 [4096, 256], P(('batch', 'mp'))
The draws below stay inside these ranges and needn't reach their ends.
Inputs may be any that keep to these rules, and one draw needn't show every extreme that they name: `lengths`: some series has 32 live steps in every draw. obs_steps[i, j] is at most lengths[i].
All inputs are finite; a program needn't handle non-finite values.
Results may differ from the reference program's by a relative error of at most 0.0019.
Values may be sent and summed in bfloat16 or wider, within the bound.
A program may use at most 64 MiB of HBM per device.

```python
import math
import jax
import jax.numpy as jnp
from jax import lax

L = 256
H = 1024
P_SIZE = 128
OBS = 8
S_STEPS = 32
ROWS_DEV = 128
SERIES = 4096


def length_table(key):
    block_count = SERIES // ROWS_DEV
    key_ceiling, key_choose, key_length, key_place = jax.random.split(jax.random.fold_in(key, 11), 4)
    ceilings = jax.random.randint(key_ceiling, (block_count,), S_STEPS // 4, S_STEPS + 1)
    chosen = jax.random.randint(key_choose, (), 0, block_count)
    ceilings = jnp.where(jnp.arange(block_count) == chosen, S_STEPS, ceilings)
    per_row = jnp.repeat(ceilings, ROWS_DEV, total_repeat_length=SERIES)
    drawn = jax.random.randint(key_length, (SERIES,), 1, per_row + 1)
    places = jax.random.randint(key_place, (block_count,), 0, ROWS_DEV)
    topmost = jnp.arange(SERIES) % ROWS_DEV == jnp.repeat(places, ROWS_DEV, total_repeat_length=SERIES)
    return jnp.where(topmost, per_row, drawn).astype(jnp.int32)


def draw_lengths(key, part):
    return length_table(key)


def draw_obs_steps(key, part):
    table = length_table(key)
    picks = jax.random.randint(jax.random.fold_in(key, 23), (SERIES, OBS), 1, table[:, None] + 1)
    return picks.astype(jnp.int32)


def levels(rng, shape, cuts, smallest, top_value):
    level, own = 1.0, jax.random.fold_in(rng, 6)
    for axis_at, blocks in cuts:
        steps = jnp.exp(jax.random.uniform(jax.random.fold_in(own, axis_at), (blocks,), jnp.float32, smallest / len(cuts), top_value / len(cuts)))
        level = level * jnp.repeat(steps, shape[axis_at] // blocks).reshape([-1 if axis == axis_at else 1 for axis in range(len(shape))])
    return level


def gaussian(own_key, extent, spread, bound, cuts=(), kind=jnp.bfloat16):
    gain = levels(own_key, extent, cuts, -0.22, 0.18) if cuts else 1.0
    values = jax.random.normal(own_key, extent, jnp.float32) * spread * gain
    return jnp.minimum(jnp.maximum(values, -bound), bound).astype(kind)


def setup_inputs(seed: int = 0) -> dict:
    key_list = jax.random.split(jax.random.key(seed), 14)
    init_state = gaussian(key_list[0], (SERIES, L), 1.0, 6.0, ((0, 32),), jnp.float32)
    brownian = gaussian(key_list[1], (S_STEPS, SERIES, L), 1.0, 6.0, ((1, 32),))
    step_size = jnp.clip(jnp.exp(math.log(0.1) - 1.609438 * jax.random.uniform(key_list[2], (SERIES,), jnp.float32) ** levels(key_list[2], (SERIES,), ((0, 32),), -0.2, 0.2)), 0.02, 0.1)
    lengths = draw_lengths(jax.random.fold_in(key_list[13], 71), 0)
    obs_steps = draw_obs_steps(jax.random.fold_in(key_list[13], 71), 0)
    observed = gaussian(key_list[5], (SERIES, OBS, P_SIZE), 1.0, 6.0, ((0, 32),))
    w_in = gaussian(key_list[6], (L, H), L ** -0.5, 0.375, ((1, 4),))
    b_in = gaussian(key_list[7], (H,), 0.5, 3.0, ((0, 4),))
    w_out = gaussian(key_list[8], (H, L), H ** -0.5, 0.1875, ((0, 4),))
    b_out = gaussian(key_list[9], (L,), 1.0, 4.0, (), jnp.float32)
    decoder = gaussian(key_list[10], (L, P_SIZE), L ** -0.5, 0.375)
    prior_rate = jnp.clip(jnp.exp(jax.random.uniform(key_list[11], (L,), jnp.float32, math.log(0.1), math.log(2.0))), 0.1, 2.0)
    diffusion = jnp.clip(jax.random.uniform(key_list[12], (L,), jnp.float32, 0.7, 1.4), 0.7, 1.4)
    return dict(init_state=init_state, brownian=brownian, step_size=step_size, lengths=lengths, obs_steps=obs_steps, observed=observed, w_in=w_in, b_in=b_in, w_out=w_out, b_out=b_out, decoder=decoder, prior_rate=prior_rate, diffusion=diffusion)


def block_terms(block_init, block_noise, block_step, block_lengths, block_obs, block_observed, w_in, b_in, w_out, b_out, decoder, prior_rate, diffusion):
    row_count = block_init.shape[0]
    num_steps = block_noise.shape[0]
    live_mask = (jnp.arange(num_steps, dtype=jnp.int32)[:, None] < block_lengths[None, :]).astype(jnp.float32)
    step_col = block_step[:, None]
    root_col = jnp.sqrt(block_step)[:, None]
    bias_in = b_in.astype(jnp.float32)

    def forward(loop_state, inputs):
        current, kl_sum = loop_state
        increment, live_now = inputs
        activity = jnp.tanh(jnp.dot(current.astype(jnp.bfloat16), w_in, preferred_element_type=jnp.float32) + bias_in).astype(jnp.bfloat16)
        drift_now = jnp.dot(activity, w_out, preferred_element_type=jnp.float32) + b_out
        residual = (drift_now + prior_rate * current) / diffusion
        kl_sum = kl_sum + live_now * 0.5 * block_step * lax.optimization_barrier(jnp.sum(residual * residual, axis=1))
        following = current + live_now[:, None] * (step_col * drift_now + diffusion * root_col * increment.astype(jnp.float32))
        return ((following, kl_sum), (current, activity, residual))
    (last_state, kl_total), (visited, activities, residuals) = lax.scan(forward, (block_init, jnp.zeros((row_count,), jnp.float32)), (block_noise, live_mask))
    trajectory = jnp.concatenate([visited, last_state[None]], axis=0)
    picked = trajectory[block_obs, jnp.arange(row_count, dtype=jnp.int32)[:, None]]
    picked_round = picked.astype(jnp.bfloat16).reshape(-1, picked.shape[2])
    flat_obs = block_observed.reshape(-1, block_observed.shape[2]).astype(jnp.float32)
    misfit = jnp.dot(picked_round, decoder, preferred_element_type=jnp.float32) - flat_obs
    loglik = -0.5 * lax.optimization_barrier(jnp.sum((misfit * misfit).reshape(row_count, -1), axis=1))
    misfit_round = misfit.astype(jnp.bfloat16)
    decoder_grad = jnp.dot(picked_round.T, misfit_round, preferred_element_type=jnp.float32)
    misfit_back = jnp.dot(misfit_round, decoder.T, preferred_element_type=jnp.float32).reshape(row_count, block_obs.shape[1], -1)
    onehot = (block_obs[:, :, None] == jnp.arange(num_steps + 1, dtype=jnp.int32)[None, None, :]).astype(jnp.float32)
    obs_back = jnp.einsum('bjs,bjl->sbl', onehot, misfit_back, precision=lax.Precision.HIGHEST)

    def backward(loop_state, inputs):
        cotangent, sum_w_in, sum_b_in, sum_w_out, sum_b_out = loop_state
        current, activity, residual, live_now, obs_here = inputs
        factor = (live_now * block_step)[:, None]
        scaled = residual / diffusion
        update = factor * (cotangent + scaled)
        update_round = update.astype(jnp.bfloat16)
        activity_value = activity.astype(jnp.float32)
        pre_grad = jnp.dot(update_round, w_out.T, preferred_element_type=jnp.float32) * (1.0 - activity_value * activity_value)
        pre_round = pre_grad.astype(jnp.bfloat16)
        cotangent = cotangent + factor * prior_rate * scaled + jnp.dot(pre_round, w_in.T, preferred_element_type=jnp.float32) + obs_here
        sum_w_in = sum_w_in + jnp.dot(current.astype(jnp.bfloat16).T, pre_round, preferred_element_type=jnp.float32)
        sum_b_in = sum_b_in + lax.optimization_barrier(jnp.sum(pre_grad, axis=0))
        sum_w_out = sum_w_out + jnp.dot(activity.T, update_round, preferred_element_type=jnp.float32)
        sum_b_out = sum_b_out + lax.optimization_barrier(jnp.sum(update, axis=0))
        return ((cotangent, sum_w_in, sum_b_in, sum_w_out, sum_b_out), None)
    start_back = (obs_back[num_steps], jnp.zeros(w_in.shape, jnp.float32), jnp.zeros((w_in.shape[1],), jnp.float32), jnp.zeros(w_out.shape, jnp.float32), jnp.zeros((w_out.shape[1],), jnp.float32))
    (cotangent, sum_w_in, sum_b_in, sum_w_out, sum_b_out), _ = lax.scan(backward, start_back, (visited, activities, residuals, live_mask, obs_back[:num_steps]), reverse=True)
    divisor = (L * block_lengths + P_SIZE * OBS).astype(jnp.float32)
    elbo_rows = (loglik - kl_total) / divisor
    return (elbo_rows, cotangent, jnp.sum(loglik), jnp.sum(kl_total), sum_w_in, sum_b_in, sum_w_out, sum_b_out, decoder_grad)

def reference(init_state, brownian, step_size, lengths, obs_steps, observed, w_in, b_in, w_out, b_out, decoder, prior_rate, diffusion):
    block_count = SERIES // ROWS_DEV
    blocked = (init_state.reshape(block_count, ROWS_DEV, L), jnp.transpose(brownian.reshape(S_STEPS, block_count, ROWS_DEV, L), (1, 0, 2, 3)), step_size.reshape(block_count, ROWS_DEV), lengths.reshape(block_count, ROWS_DEV), obs_steps.reshape(block_count, ROWS_DEV, OBS), observed.reshape(block_count, ROWS_DEV, OBS, P_SIZE))
    zero_totals = (jnp.zeros((L, H), jnp.float32), jnp.zeros((H,), jnp.float32), jnp.zeros((H, L), jnp.float32), jnp.zeros((L,), jnp.float32), jnp.zeros((L, P_SIZE), jnp.float32), jnp.zeros((), jnp.float32), jnp.zeros((), jnp.float32))

    def visit(totals, pieces):
        outcome = block_terms(pieces[0], pieces[1], pieces[2], pieces[3], pieces[4], pieces[5], w_in, b_in, w_out, b_out, decoder, prior_rate, diffusion)
        elbo_rows, init_grad, loglik_sum, kl_sum, sum_w_in, sum_b_in, sum_w_out, sum_b_out, decoder_grad = outcome
        fresh = (sum_w_in, sum_b_in, sum_w_out, sum_b_out, decoder_grad, loglik_sum, kl_sum)
        totals = tuple((first + second for first, second in zip(totals, fresh)))
        return (totals, (elbo_rows, init_grad))
    totals, (elbo_rows, init_grads) = lax.scan(visit, zero_totals, blocked)
    elbo_series = elbo_rows.reshape(SERIES)
    grad_init = init_grads.reshape(SERIES, L)
    scores = jnp.stack([totals[5] / SERIES, totals[6] / SERIES])
    return (elbo_series, scores, totals[0] / SERIES, totals[1] / SERIES, totals[2] / SERIES, totals[3] / SERIES, totals[4] / SERIES, grad_init)
```

```python
import jax
import jax.numpy as jnp
from jax import lax
from jax.experimental import pallas as pl
from jax.experimental.pallas import tpu as pltpu
from jax.sharding import PartitionSpec as P

F32 = jnp.float32
BF16 = jnp.bfloat16
NT = (((1,), (1,)), ((), ()))


def dot(a, b):
    return jnp.dot(a, b, preferred_element_type=F32)


def dot_nt(a, b):
    return lax.dot_general(a, b, NT, preferred_element_type=F32)


def fold(value):
    return value.reshape(-1, 8, value.shape[1]).sum(axis=0)


def core_kernel(
    init_ref,
    noise_ref,
    step_ref,
    length_ref,
    obs_ref,
    seen_ref,
    w_in_ref,
    b_in_ref,
    w_out_ref,
    b_out_ref,
    dec_ref,
    rate_ref,
    diff_ref,
    elbo_ref,
    grads_ref,
    small_ref,
    dec_grad_ref,
    cot_ref,
    x_ref,
    xt_ref,
    ut_ref,
    act_ref,
    pre_ref,
    scaled_ref,
    pick_ref,
    obs_wide_ref,
    dt_ref,
    root_ref,
    len_ref,
    state_ref,
    kl_ref,
    sum_b_in_ref,
    sum_b_out_ref,
    miss_ref,
):
    rows, width = init_ref.shape
    steps = noise_ref.shape[0]
    hidden = w_in_ref.shape[1]
    seen_count = obs_ref.shape[0]
    seen_width = dec_ref.shape[1]
    chunks = hidden // width

    def column(row):
        return jnp.broadcast_to(row, (rows, rows)).T

    dt_ref[...] = column(step_ref[...])
    root_ref[...] = jnp.sqrt(dt_ref[...])
    len_ref[...] = column(length_ref[...])
    for j in range(seen_count):
        obs_wide_ref[j] = column(obs_ref[j : j + 1, :])
    pick_ref[...] = jnp.zeros_like(pick_ref)
    kl_ref[...] = jnp.zeros_like(kl_ref)
    sum_b_in_ref[...] = jnp.zeros_like(sum_b_in_ref)
    sum_b_out_ref[...] = jnp.zeros_like(sum_b_out_ref)
    state_ref[...] = init_ref[...]
    x_ref[0] = init_ref[...].astype(BF16)

    def both(value):
        return jnp.concatenate([value] * (width // rows), axis=1)

    def forward(k, carry):
        x = x_ref[k]
        drift = jnp.broadcast_to(b_out_ref[...], (rows, width))
        for n in range(chunks):
            cols = slice(n * width, (n + 1) * width)
            act = jnp.tanh(dot(x, w_in_ref[:, cols]) + b_in_ref[:, cols]).astype(BF16)
            act_ref[n, pl.ds(k * rows, rows), :] = act
            drift = drift + dot(act, w_out_ref[cols, :])
        state = state_ref[...]
        inv = 1.0 / diff_ref[...]
        live = k < len_ref[...]
        factor = both(jnp.where(live, dt_ref[...], 0.0))
        root = both(jnp.where(live, root_ref[...], 0.0))
        residual = (drift + rate_ref[...] * state) * inv
        kl_ref[...] += factor * residual * residual
        scaled_ref[k] = residual * inv
        following = state + (
            factor * drift + diff_ref[...] * root * noise_ref[k].astype(F32)
        )
        state_ref[...] = following
        rounded = following.astype(BF16)
        x_ref[k + 1] = rounded
        xt_ref[:, pl.ds(pl.multiple_of(k * rows, rows), rows)] = x.T
        seen = dot(rounded, dec_ref[...])
        for j in range(seen_count):
            pick_ref[j] = jnp.where(obs_wide_ref[j] == k + 1, seen, pick_ref[j])
        return carry

    lax.fori_loop(0, steps, forward, 0)

    square = jnp.zeros((rows, seen_width), F32)
    for j in range(seen_count):
        misfit = pick_ref[j] - seen_ref[j].astype(F32)
        square = square + misfit * misfit
        pick_ref[j] = misfit.astype(BF16).astype(F32)
    loglik = -0.5 * jnp.sum(square.T, axis=0, keepdims=True)
    kl_half = kl_ref[:, :rows]
    for part in range(1, width // rows):
        kl_half = kl_half + kl_ref[:, part * rows : (part + 1) * rows]
    kl_row = 0.5 * jnp.sum(kl_half.T, axis=0, keepdims=True)
    divisor = (width * length_ref[...] + seen_width * seen_count).astype(F32)
    elbo_ref[...] = (loglik - kl_row) / divisor

    cot_ref[...] = jnp.zeros_like(cot_ref)

    def backward(index, carry):
        k = steps - 1 - index
        total = jnp.zeros((rows, seen_width), F32)
        for j in range(seen_count):
            total = total + jnp.where(obs_wide_ref[j] == k + 1, pick_ref[j], 0.0)
        high = total.astype(BF16)
        low = (total - high.astype(F32)).astype(BF16)
        miss_ref[pl.ds(k * rows, rows), :seen_width] = high
        miss_ref[pl.ds(k * rows, rows), seen_width:] = low
        obs_back = dot_nt(high, dec_ref[...]) + dot_nt(low, dec_ref[...])
        cot = cot_ref[...] + obs_back
        scaled = scaled_ref[k]
        factor = both(jnp.where(k < len_ref[...], dt_ref[...], 0.0))
        update = factor * (cot + scaled)
        rounded = update.astype(BF16)
        ut_ref[:, pl.ds(pl.multiple_of(k * rows, rows), rows)] = rounded.T
        sum_b_out_ref[...] += fold(update)
        cot = cot + factor * rate_ref[...] * scaled
        for n in range(chunks):
            cols = slice(n * width, (n + 1) * width)
            act = act_ref[n, pl.ds(k * rows, rows), :].astype(F32)
            pre = dot_nt(rounded, w_out_ref[cols, :]) * (1.0 - act * act)
            sum_b_in_ref[n] += fold(pre)
            pre_round = pre.astype(BF16)
            pre_ref[n, pl.ds(k * rows, rows), :] = pre_round
            cot = cot + dot_nt(pre_round, w_in_ref[:, cols])
        cot_ref[...] = cot
        return carry

    lax.fori_loop(0, steps, backward, 0)

    def gradients(n, carry):
        grads_ref[n, :width, :] = dot(xt_ref[...], pre_ref[n])
        grads_ref[n, width:, :] = dot(ut_ref[...], act_ref[n]).T
        return carry

    lax.fori_loop(0, chunks, gradients, 0)

    dec_grad = jnp.zeros((width, 2 * seen_width), F32)
    dec_grad = dec_grad + dot(xt_ref[:, rows:], miss_ref[: (steps - 1) * rows, :])
    last = lax.dot_general(
        x_ref[steps],
        miss_ref[(steps - 1) * rows :, :],
        (((0,), (0,)), ((), ())),
        preferred_element_type=F32,
    )
    dec_grad = dec_grad + last
    dec_grad_ref[...] = dec_grad[:, :seen_width] + dec_grad[:, seen_width:]
    for n in range(chunks):
        small_ref[n : n + 1, :] = jnp.sum(sum_b_in_ref[n], axis=0, keepdims=True)
    small_ref[chunks : chunks + 1, :] = jnp.sum(sum_b_out_ref[...], axis=0, keepdims=True)
    small_ref[chunks + 1 : chunks + 2, :rows] = loglik
    small_ref[chunks + 1 : chunks + 2, rows:] = kl_row
    small_ref[chunks + 2 :, :] = jnp.zeros((small_ref.shape[0] - chunks - 2, width), F32)


def core(init, noise, step, length, obs, seen, w_in, b_in, w_out, b_out, dec, rate, diff):
    rows, width = init.shape
    steps = noise.shape[0]
    hidden = w_in.shape[1]
    seen_count, seen_width = seen.shape[0], dec.shape[1]
    chunks = hidden // width
    vmem = pl.BlockSpec(memory_space=pltpu.VMEM)
    small_rows = -(-(chunks + 2) // 8) * 8
    out = [
        jax.ShapeDtypeStruct((1, rows), F32),
        jax.ShapeDtypeStruct((chunks, 2 * width, width), F32),
        jax.ShapeDtypeStruct((small_rows, width), F32),
        jax.ShapeDtypeStruct(dec.shape, F32),
        jax.ShapeDtypeStruct((rows, width), F32),
    ]
    scratch = [
        pltpu.VMEM((steps + 1, rows, width), BF16),
        pltpu.VMEM((width, steps * rows), BF16),
        pltpu.VMEM((width, steps * rows), BF16),
        pltpu.VMEM((chunks, steps * rows, width), BF16),
        pltpu.VMEM((chunks, steps * rows, width), BF16),
        pltpu.VMEM((steps, rows, width), F32),
        pltpu.VMEM((seen_count, rows, seen_width), F32),
        pltpu.VMEM((seen_count, rows, rows), jnp.int32),
        pltpu.VMEM((rows, rows), F32),
        pltpu.VMEM((rows, rows), F32),
        pltpu.VMEM((rows, rows), jnp.int32),
        pltpu.VMEM((rows, width), F32),
        pltpu.VMEM((rows, width), F32),
        pltpu.VMEM((chunks, 8, width), F32),
        pltpu.VMEM((8, width), F32),
        pltpu.VMEM((steps * rows, 2 * seen_width), BF16),
    ]
    return pl.pallas_call(
        core_kernel,
        out_shape=out,
        in_specs=[vmem] * 13,
        out_specs=[vmem] * 5,
        scratch_shapes=scratch,
        compiler_params=pltpu.CompilerParams(vmem_limit_bytes=60 * 1024 * 1024),
        name="sde",
    )(init, noise, step, length, obs, seen, w_in, b_in, w_out, b_out, dec, rate, diff)


def on_device(
    init_state,
    brownian,
    step_size,
    lengths,
    obs_steps,
    observed,
    w_in,
    b_in,
    w_out,
    b_out,
    decoder,
    prior_rate,
    diffusion,
):
    w_in_all, w_out_all, b_in_all = (
        lax.all_gather(w_in, "mp", axis=1, tiled=True),
        lax.all_gather(w_out, "mp", axis=0, tiled=True),
        lax.all_gather(b_in, "mp", axis=0, tiled=True),
    )
    rows, width = init_state.shape
    chunks = w_in_all.shape[1] // width
    elbo, grads, small, dec_grad, cot = core(
        init_state,
        brownian,
        step_size[None, :],
        lengths[None, :],
        obs_steps.T,
        observed.transpose(1, 0, 2),
        w_in_all,
        b_in_all.astype(F32)[None, :],
        w_out_all,
        b_out[None, :],
        decoder,
        prior_rate[None, :],
        diffusion[None, :],
    )
    total = rows * lax.axis_size("batch") * lax.axis_size("mp")
    mine = lax.axis_index("mp")
    grads = lax.psum_scatter(grads, "mp", scatter_dimension=0, tiled=True)[0]
    grads = lax.psum(grads, "batch") / total
    small, dec_grad = lax.psum((small, dec_grad), ("batch", "mp"))
    scores = jnp.stack([jnp.sum(small[chunks + 1, :rows]), jnp.sum(small[chunks + 1, rows:])])
    own_b_in = lax.dynamic_slice_in_dim(small, mine, 1, 0)[0]
    return (
        elbo[0],
        scores / total,
        grads[:width],
        own_b_in / total,
        grads[width:],
        small[chunks] / total,
        dec_grad / total,
        cot,
    )


def solution(mesh):
    both = ("batch", "mp")
    placed = (
        P(both, None),
        P(None, both, None),
        P(both),
        P(both),
        P(both, None),
        P(both, None, None),
        P(None, "mp"),
        P("mp"),
        P("mp", None),
        P(),
        P(),
        P(),
        P(),
    )
    return jax.shard_map(
        on_device,
        mesh=mesh,
        in_specs=placed,
        out_specs=(
            P(both),
            P(),
            P(None, "mp"),
            P("mp"),
            P("mp", None),
            P(),
            P(),
            P(both, None),
        ),
        check_vma=False,
    )
```

```python
import jax
import jax.numpy as jnp
from jax import lax
from jax.experimental import pallas as pl
from jax.experimental.pallas import tpu as pltpu
from jax.sharding import PartitionSpec as P

F32 = jnp.float32
BF16 = jnp.bfloat16
NT = (((1,), (1,)), ((), ()))


def dot(a, b):
    return jnp.dot(a, b, preferred_element_type=F32)


def dot_nt(a, b):
    return lax.dot_general(a, b, NT, preferred_element_type=F32)


def fold(value):
    return value.reshape(-1, 8, value.shape[1]).sum(axis=0)


def core_kernel(
    init_ref,
    noise_ref,
    step_ref,
    length_ref,
    obs_ref,
    seen_ref,
    w_in_ref,
    b_in_ref,
    w_out_ref,
    b_out_ref,
    dec_ref,
    rate_ref,
    diff_ref,
    elbo_ref,
    grads_ref,
    cot_ref,
    x_ref,
    xt_ref,
    ut_ref,
    act_ref,
    pre_ref,
    scaled_ref,
    pick_ref,
    obs_wide_ref,
    dt_ref,
    root_ref,
    len_ref,
    state_ref,
    kl_ref,
    sum_b_in_ref,
    sum_b_out_ref,
    miss_ref,
):
    rows, width = init_ref.shape
    steps = noise_ref.shape[0]
    seen_count = obs_ref.shape[0]
    seen_width = dec_ref.shape[1]
    chunks = w_in_ref.shape[0]

    def column(row):
        return jnp.broadcast_to(row, (rows, rows)).T

    dt_ref[...] = column(step_ref[...])
    root_ref[...] = jnp.sqrt(dt_ref[...])
    len_ref[...] = column(length_ref[...])
    for j in range(seen_count):
        obs_wide_ref[j] = column(obs_ref[j : j + 1, :])
    pick_ref[...] = jnp.zeros_like(pick_ref)
    kl_ref[...] = jnp.zeros_like(kl_ref)
    sum_b_in_ref[...] = jnp.zeros_like(sum_b_in_ref)
    sum_b_out_ref[...] = jnp.zeros_like(sum_b_out_ref)
    state_ref[...] = init_ref[...]
    x_ref[0] = init_ref[...].astype(BF16)

    def both(value):
        return jnp.concatenate([value] * (width // rows), axis=1)

    def forward(k, carry):
        x = x_ref[k]
        drift = jnp.broadcast_to(b_out_ref[...], (rows, width))
        for n in range(chunks):
            act = jnp.tanh(dot(x, w_in_ref[n]) + b_in_ref[n, :1, :]).astype(BF16)
            act_ref[n, pl.ds(k * rows, rows), :] = act
            drift = drift + dot(act, w_out_ref[n])
        state = state_ref[...]
        inv = 1.0 / diff_ref[...]
        live = k < len_ref[...]
        factor = both(jnp.where(live, dt_ref[...], 0.0))
        root = both(jnp.where(live, root_ref[...], 0.0))
        residual = (drift + rate_ref[...] * state) * inv
        kl_ref[...] += factor * residual * residual
        scaled_ref[k] = residual * inv
        following = state + (
            factor * drift + diff_ref[...] * root * noise_ref[k].astype(F32)
        )
        state_ref[...] = following
        rounded = following.astype(BF16)
        x_ref[k + 1] = rounded
        xt_ref[:, pl.ds(pl.multiple_of(k * rows, rows), rows)] = x.T
        seen = dot(rounded, dec_ref[...])
        for j in range(seen_count):
            pick_ref[j] = jnp.where(obs_wide_ref[j] == k + 1, seen, pick_ref[j])
        return carry

    lax.fori_loop(0, steps, forward, 0)

    square = jnp.zeros((rows, seen_width), F32)
    for j in range(seen_count):
        misfit = pick_ref[j] - seen_ref[j].astype(F32)
        square = square + misfit * misfit
        pick_ref[j] = misfit.astype(BF16).astype(F32)
    loglik = -0.5 * jnp.sum(square.T, axis=0, keepdims=True)
    kl_half = kl_ref[:, :rows]
    for part in range(1, width // rows):
        kl_half = kl_half + kl_ref[:, part * rows : (part + 1) * rows]
    kl_row = 0.5 * jnp.sum(kl_half.T, axis=0, keepdims=True)
    divisor = (width * length_ref[...] + seen_width * seen_count).astype(F32)
    elbo_ref[...] = (loglik - kl_row) / divisor

    cot_ref[...] = jnp.zeros_like(cot_ref)

    def backward(index, carry):
        k = steps - 1 - index
        total = jnp.zeros((rows, seen_width), F32)
        for j in range(seen_count):
            total = total + jnp.where(obs_wide_ref[j] == k + 1, pick_ref[j], 0.0)
        high = total.astype(BF16)
        low = (total - high.astype(F32)).astype(BF16)
        miss_ref[pl.ds(k * rows, rows), :seen_width] = high
        miss_ref[pl.ds(k * rows, rows), seen_width:] = low
        obs_back = dot_nt(high, dec_ref[...]) + dot_nt(low, dec_ref[...])
        cot = cot_ref[...] + obs_back
        scaled = scaled_ref[k]
        factor = both(jnp.where(k < len_ref[...], dt_ref[...], 0.0))
        update = factor * (cot + scaled)
        rounded = update.astype(BF16)
        ut_ref[:, pl.ds(pl.multiple_of(k * rows, rows), rows)] = rounded.T
        sum_b_out_ref[...] += fold(update)
        cot = cot + factor * rate_ref[...] * scaled
        for n in range(chunks):
            act = act_ref[n, pl.ds(k * rows, rows), :].astype(F32)
            pre = dot_nt(rounded, w_out_ref[n]) * (1.0 - act * act)
            sum_b_in_ref[n] += fold(pre)
            pre_round = pre.astype(BF16)
            pre_ref[n, pl.ds(k * rows, rows), :] = pre_round
            cot = cot + dot_nt(pre_round, w_in_ref[n])
        cot_ref[...] = cot
        return carry

    lax.fori_loop(0, steps, backward, 0)

    def gradients(n, carry):
        grads_ref[n, :width, :] = dot(xt_ref[...], pre_ref[n])
        grads_ref[n, width : 2 * width, :] = dot(ut_ref[...], act_ref[n]).T
        return carry

    lax.fori_loop(0, chunks, gradients, 0)

    dec_grad = jnp.zeros((width, 2 * seen_width), F32)
    dec_grad = dec_grad + dot(xt_ref[:, rows:], miss_ref[: (steps - 1) * rows, :])
    last = lax.dot_general(
        x_ref[steps],
        miss_ref[(steps - 1) * rows :, :],
        (((0,), (0,)), ((), ())),
        preferred_element_type=F32,
    )
    dec_grad = dec_grad + last
    dec_grad = dec_grad[:, :seen_width] + dec_grad[:, seen_width:]
    lanes = width // seen_width
    share = width // chunks
    tail = 2 * width
    line = tail + share // lanes
    for n in range(chunks):
        pieces = [
            dec_grad[n * share + m * share // lanes : n * share + (m + 1) * share // lanes, :]
            for m in range(lanes)
        ]
        grads_ref[n, tail:line, :] = jnp.concatenate(pieces, axis=1)
        grads_ref[n, line:, :] = jnp.zeros((grads_ref.shape[1] - line, width), F32)
        grads_ref[n, line : line + 1, :] = jnp.sum(sum_b_in_ref[n], axis=0, keepdims=True)
        grads_ref[n, line + 1 : line + 2, :] = jnp.sum(
            sum_b_out_ref[...], axis=0, keepdims=True
        )
        grads_ref[n, line + 2 : line + 3, :rows] = loglik
        grads_ref[n, line + 2 : line + 3, rows : 2 * rows] = kl_row


def core(grad_rows, init, noise, step, length, obs, seen, w_in, b_in, w_out, b_out, dec, rate, diff):
    rows, width = init.shape
    steps = noise.shape[0]
    seen_count, seen_width = seen.shape[0], dec.shape[1]
    chunks = w_in.shape[0]
    vmem = pl.BlockSpec(memory_space=pltpu.VMEM)
    out = [
        jax.ShapeDtypeStruct((1, rows), F32),
        jax.ShapeDtypeStruct((chunks, grad_rows, width), F32),
        jax.ShapeDtypeStruct((rows, width), F32),
    ]
    scratch = [
        pltpu.VMEM((steps + 1, rows, width), BF16),
        pltpu.VMEM((width, steps * rows), BF16),
        pltpu.VMEM((width, steps * rows), BF16),
        pltpu.VMEM((chunks, steps * rows, width), BF16),
        pltpu.VMEM((chunks, steps * rows, width), BF16),
        pltpu.VMEM((steps, rows, width), F32),
        pltpu.VMEM((seen_count, rows, seen_width), F32),
        pltpu.VMEM((seen_count, rows, rows), jnp.int32),
        pltpu.VMEM((rows, rows), F32),
        pltpu.VMEM((rows, rows), F32),
        pltpu.VMEM((rows, rows), jnp.int32),
        pltpu.VMEM((rows, width), F32),
        pltpu.VMEM((rows, width), F32),
        pltpu.VMEM((chunks, 8, width), F32),
        pltpu.VMEM((8, width), F32),
        pltpu.VMEM((steps * rows, 2 * seen_width), BF16),
    ]
    return pl.pallas_call(
        core_kernel,
        out_shape=out,
        in_specs=[vmem] * 13,
        out_specs=[vmem] * 3,
        scratch_shapes=scratch,
        compiler_params=pltpu.CompilerParams(vmem_limit_bytes=60 * 1024 * 1024),
        name="sde",
    )(init, noise, step, length, obs, seen, w_in, b_in, w_out, b_out, dec, rate, diff)


def send(source, target, send_sem, recv_sem, peer):
    return pltpu.make_async_remote_copy(
        src_ref=source,
        dst_ref=target,
        send_sem=send_sem,
        recv_sem=recv_sem,
        device_id=peer,
        device_id_type=pl.DeviceIdType.MESH,
    )


def greet(peers):
    barrier = pltpu.get_barrier_semaphore()
    for peer in peers:
        pl.semaphore_signal(barrier, inc=1, device_id=peer, device_id_type=pl.DeviceIdType.MESH)
    pl.semaphore_wait(barrier, len(peers))


def mp_places():
    mine = lax.axis_index("mp")
    chip, unit = mine // 2, mine % 2
    sibling = chip * 2 + (1 - unit)
    across = (1 - chip) * 2 + unit
    diagonal = (1 - chip) * 2 + (1 - unit)
    return mine, sibling, across, diagonal


def gather_kernel(w_in_ref, w_out_ref, b_in_ref, all_in_ref, all_out_ref, all_b_ref, bias_ref, send_sem, recv_sem):
    mine, sibling, across, diagonal = mp_places()
    batch = lax.axis_index("batch")
    to_across, to_sibling = (batch, across), (batch, sibling)
    bias_ref[...] = jnp.broadcast_to(b_in_ref[...].astype(F32), bias_ref.shape)
    greet([to_across, to_sibling])
    pairs = ((w_in_ref, all_in_ref), (w_out_ref, all_out_ref), (bias_ref, all_b_ref))
    far, near, relayed = [], [], []
    for i, (own, whole) in enumerate(pairs):
        copy = send(own, whole.at[mine], send_sem.at[0, i], recv_sem.at[0, i], to_across)
        copy.start()
        far.append(copy)
    for i, (own, whole) in enumerate(pairs):
        copy = send(own, whole.at[mine], send_sem.at[1, i], recv_sem.at[1, i], to_sibling)
        copy.start()
        near.append(copy)
    for own, whole in pairs:
        whole[mine] = own[...]
    for i, (own, whole) in enumerate(pairs):
        far[i].wait_recv()
        copy = send(
            whole.at[across], whole.at[across], send_sem.at[2, i], recv_sem.at[2, i], to_sibling
        )
        copy.start()
        relayed.append(copy)
    for copy in far:
        copy.wait_send()
    for copy in near + relayed:
        copy.wait()


def gather(w_in, w_out, b_in):
    count = lax.axis_size("mp")
    vmem = pl.BlockSpec(memory_space=pltpu.VMEM)
    return pl.pallas_call(
        gather_kernel,
        out_shape=[
            jax.ShapeDtypeStruct((count,) + w_in.shape, BF16),
            jax.ShapeDtypeStruct((count,) + w_out.shape, BF16),
            jax.ShapeDtypeStruct((count, 8, b_in.shape[1]), F32),
        ],
        in_specs=[vmem] * 3,
        out_specs=[vmem] * 3,
        scratch_shapes=[
            pltpu.VMEM((8, b_in.shape[1]), F32),
            pltpu.SemaphoreType.DMA((3, 3)),
            pltpu.SemaphoreType.DMA((3, 3)),
        ],
        compiler_params=pltpu.CompilerParams(
            collective_id=0, has_side_effects=True, vmem_limit_bytes=16 * 1024 * 1024
        ),
        name="gather_weights",
    )(w_in, w_out, b_in)


def reduce_kernel(
    members,
    total,
    share,
    grads_ref,
    w_in_ref,
    w_out_ref,
    b_in_ref,
    b_out_ref,
    dec_ref,
    scores_ref,
    near_ref,
    far_w_ref,
    far_t_ref,
    got_w_ref,
    got_t_ref,
    full_ref,
    parts_ref,
    done_ref,
    decs_ref,
    near_send,
    near_recv,
    far_send,
    far_recv,
    rs_send,
    rs_recv,
    ag_send,
    ag_recv,
    dec_send,
    dec_recv,
):
    mine, sibling, across, diagonal = mp_places()
    batch = lax.axis_index("batch")
    width = grads_ref.shape[2]
    weight_rows = 2 * width
    piece = grads_ref.shape[1] // members
    others = [(lax.rem(batch + d, members), mine) for d in range(1, members)]
    group = [(batch, sibling), (batch, across), (batch, diagonal)]
    greet(group + others)
    near = []
    for i, quarter in enumerate((diagonal, sibling)):
        copy = send(
            grads_ref.at[quarter], near_ref.at[i], near_send.at[i], near_recv.at[i], group[0]
        )
        copy.start()
        near.append(copy)
    near[0].wait_recv()
    far_w_ref[...] = (
        grads_ref[across, :weight_rows, :] + near_ref[0, :weight_rows, :]
    ).astype(BF16)
    far_t_ref[...] = grads_ref[across, weight_rows:, :] + near_ref[0, weight_rows:, :]
    far = [
        send(far_w_ref, got_w_ref, far_send.at[0], far_recv.at[0], group[1]),
        send(far_t_ref, got_t_ref, far_send.at[1], far_recv.at[1], group[1]),
    ]
    for copy in far:
        copy.start()
    near[1].wait_recv()
    full_ref[...] = grads_ref[mine] + near_ref[1]
    far[0].wait_recv()
    full_ref[:weight_rows, :] += got_w_ref[...].astype(F32)
    far[1].wait_recv()
    full_ref[weight_rows:, :] += got_t_ref[...]
    scatter = []
    for d in range(1, members):
        target = lax.rem(batch + d, members)
        copy = send(
            full_ref.at[pl.ds(pl.multiple_of(target * piece, 8), piece), :],
            parts_ref.at[d - 1],
            rs_send.at[d - 1],
            rs_recv.at[d - 1],
            others[d - 1],
        )
        copy.start()
        scatter.append(copy)
    here = pl.ds(pl.multiple_of(batch * piece, 8), piece)
    value = full_ref[here, :]
    for d in range(1, members):
        scatter[d - 1].wait_recv()
        value = value + parts_ref[d - 1]
    done_ref[here, :] = value / total
    spread = []
    for d in range(1, members):
        copy = send(
            done_ref.at[here, :],
            done_ref.at[here, :],
            ag_send.at[d - 1],
            ag_recv.at[d - 1],
            others[d - 1],
        )
        copy.start()
        spread.append(copy)
    for copy in near + far + scatter:
        copy.wait_send()
    for d in range(1, members):
        origin = lax.rem(batch + members - d, members)
        there = pl.ds(pl.multiple_of(origin * piece, 8), piece)
        send(
            done_ref.at[there, :],
            done_ref.at[there, :],
            ag_send.at[d - 1],
            ag_recv.at[d - 1],
            others[d - 1],
        ).wait_recv()
    dec_rows = decs_ref.shape[1]
    line = weight_rows + dec_rows
    exchange = []
    for i in range(3):
        copy = send(
            done_ref.at[pl.ds(weight_rows, dec_rows), :],
            decs_ref.at[mine],
            dec_send.at[i],
            dec_recv.at[i],
            group[i],
        )
        copy.start()
        exchange.append(copy)
    w_in_ref[...] = done_ref[:width, :]
    w_out_ref[...] = done_ref[width:weight_rows, :]
    decs_ref[mine] = done_ref[weight_rows:line, :]
    b_in_ref[...] = done_ref[line : line + 1, :]
    b_out_ref[...] = done_ref[line + 1 : line + 2, :]
    half = share
    scores_ref[:, 0:1] = jnp.sum(done_ref[line + 2 : line + 3, :half], axis=1, keepdims=True)
    scores_ref[:, 1:2] = jnp.sum(
        done_ref[line + 2 : line + 3, half : 2 * half], axis=1, keepdims=True
    )
    for copy in spread:
        copy.wait_send()
    for i, origin in enumerate((sibling, across, diagonal)):
        exchange[i].wait_send()
        send(
            decs_ref.at[origin], decs_ref.at[origin], dec_send.at[i], dec_recv.at[i], group[i]
        ).wait_recv()
    seen_width = dec_ref.shape[1]
    for n in range(decs_ref.shape[0]):
        for m in range(width // seen_width):
            start = (n * (width // seen_width) + m) * dec_rows
            dec_ref[start : start + dec_rows, :] = decs_ref[
                n, :, m * seen_width : (m + 1) * seen_width
            ]


def reduce_all(grads, rows, seen_width):
    quarters, grad_rows, width = grads.shape
    members = lax.axis_size("batch")
    total = rows * members * lax.axis_size("mp")
    dec_rows = width // quarters // (width // seen_width)
    tail_rows = grad_rows - 2 * width
    piece = grad_rows // members
    vmem = pl.BlockSpec(memory_space=pltpu.VMEM)
    sems = []
    for count in (2, 2, members - 1, members - 1, 3):
        sems += [pltpu.SemaphoreType.DMA((count,))] * 2

    def body(*refs):
        reduce_kernel(members, total, rows, *refs)

    return pl.pallas_call(
        body,
        out_shape=[
            jax.ShapeDtypeStruct((width, width), F32),
            jax.ShapeDtypeStruct((width, width), F32),
            jax.ShapeDtypeStruct((1, width), F32),
            jax.ShapeDtypeStruct((1, width), F32),
            jax.ShapeDtypeStruct((width, seen_width), F32),
            jax.ShapeDtypeStruct((1, 2), F32),
        ],
        in_specs=[vmem],
        out_specs=[vmem] * 6,
        scratch_shapes=[
            pltpu.VMEM((2, grad_rows, width), F32),
            pltpu.VMEM((2 * width, width), BF16),
            pltpu.VMEM((tail_rows, width), F32),
            pltpu.VMEM((2 * width, width), BF16),
            pltpu.VMEM((tail_rows, width), F32),
            pltpu.VMEM((grad_rows, width), F32),
            pltpu.VMEM((members - 1, piece, width), F32),
            pltpu.VMEM((grad_rows, width), F32),
            pltpu.VMEM((quarters, dec_rows, width), F32),
        ]
        + sems,
        compiler_params=pltpu.CompilerParams(
            collective_id=1, has_side_effects=True, vmem_limit_bytes=32 * 1024 * 1024
        ),
        name="reduce_grads",
    )(grads)


def on_device(
    init_state,
    brownian,
    step_size,
    lengths,
    obs_steps,
    observed,
    w_in,
    b_in,
    w_out,
    b_out,
    decoder,
    prior_rate,
    diffusion,
):
    rows, width = init_state.shape
    seen_width = decoder.shape[1]
    w_in_all, w_out_all, b_in_all = gather(w_in, w_out, b_in[None, :])
    unit = 8 * lax.axis_size("batch")
    need = 2 * width + width // lax.axis_size("mp") * seen_width // width + 3
    elbo, grads, cot = core(
        -(-need // unit) * unit,
        init_state,
        brownian,
        step_size[None, :],
        lengths[None, :],
        obs_steps.T,
        observed.transpose(1, 0, 2),
        w_in_all,
        b_in_all,
        w_out_all,
        b_out[None, :],
        decoder,
        prior_rate[None, :],
        diffusion[None, :],
    )
    own_w_in, own_w_out, own_b_in, b_out_grad, dec_grad, scores = reduce_all(
        grads, rows, seen_width
    )
    return (
        elbo[0],
        scores[0],
        own_w_in,
        own_b_in[0],
        own_w_out,
        b_out_grad[0],
        dec_grad,
        cot,
    )


def solution(mesh):
    both = ("batch", "mp")
    placed = (
        P(both, None),
        P(None, both, None),
        P(both),
        P(both),
        P(both, None),
        P(both, None, None),
        P(None, "mp"),
        P("mp"),
        P("mp", None),
        P(),
        P(),
        P(),
        P(),
    )
    return jax.shard_map(
        on_device,
        mesh=mesh,
        in_specs=placed,
        out_specs=(
            P(both),
            P(),
            P(None, "mp"),
            P("mp"),
            P("mp", None),
            P(),
            P(),
            P(both, None),
        ),
        check_vma=False,
    )
```

```python
import jax
import jax.numpy as jnp
from jax import lax
from jax.experimental import pallas as pl
from jax.experimental.pallas import tpu as pltpu
from jax.sharding import PartitionSpec as P

F32 = jnp.float32
BF16 = jnp.bfloat16
NT = (((1,), (1,)), ((), ()))


def dot(a, b):
    return jnp.dot(a, b, preferred_element_type=F32)


def dot_nt(a, b):
    return lax.dot_general(a, b, NT, preferred_element_type=F32)


def fold(value):
    return value.reshape(-1, 8, value.shape[1]).sum(axis=0)


def core_kernel(
    init_ref,
    noise_ref,
    step_ref,
    length_ref,
    obs_ref,
    seen_ref,
    w_in_ref,
    b_in_ref,
    w_out_ref,
    b_out_ref,
    dec_ref,
    rate_ref,
    diff_ref,
    elbo_ref,
    grads_ref,
    cot_ref,
    x_ref,
    xt_ref,
    ut_ref,
    act_ref,
    pre_ref,
    scaled_ref,
    pick_ref,
    obs_wide_ref,
    dt_ref,
    root_ref,
    len_ref,
    state_ref,
    kl_ref,
    sum_b_in_ref,
    sum_b_out_ref,
    miss_ref,
    target_ref,
):
    rows, width = init_ref.shape
    steps = noise_ref.shape[0]
    seen_count = obs_ref.shape[0]
    seen_width = dec_ref.shape[1]
    chunks = w_in_ref.shape[0]

    def column(row):
        return jnp.broadcast_to(row, (rows, rows)).T

    dt_ref[...] = column(step_ref[...])
    root_ref[...] = jnp.sqrt(dt_ref[...])
    len_ref[...] = column(length_ref[...])
    for j in range(seen_count):
        obs_wide_ref[j] = column(obs_ref[j : j + 1, :])
    target_ref[...] = seen_ref[...].astype(F32).reshape(target_ref.shape)
    pick_ref[...] = jnp.zeros_like(pick_ref)
    kl_ref[...] = jnp.zeros_like(kl_ref)
    sum_b_in_ref[...] = jnp.zeros_like(sum_b_in_ref)
    sum_b_out_ref[...] = jnp.zeros_like(sum_b_out_ref)
    state_ref[...] = init_ref[...]
    x_ref[0] = init_ref[...].astype(BF16)

    def both(value):
        return jnp.concatenate([value] * (width // rows), axis=1)

    def forward(k, carry):
        x = x_ref[k]
        drift = jnp.broadcast_to(b_out_ref[...], (rows, width))
        for n in range(chunks):
            act = jnp.tanh(dot(x, w_in_ref[n]) + b_in_ref[n, :1, :]).astype(BF16)
            act_ref[n, pl.ds(k * rows, rows), :] = act
            drift = drift + dot(act, w_out_ref[n])
        state = state_ref[...]
        inv = 1.0 / diff_ref[...]
        live = k < len_ref[...]
        factor = both(jnp.where(live, dt_ref[...], 0.0))
        root = both(jnp.where(live, root_ref[...], 0.0))
        residual = (drift + rate_ref[...] * state) * inv
        kl_ref[...] += factor * residual * residual
        scaled_ref[k] = residual * inv
        following = state + (
            factor * drift + diff_ref[...] * root * noise_ref[k].astype(F32)
        )
        state_ref[...] = following
        rounded = following.astype(BF16)
        x_ref[k + 1] = rounded
        xt_ref[:, pl.ds(pl.multiple_of(k * rows, rows), rows)] = x.T
        seen = dot(rounded, dec_ref[...])
        for j in range(seen_count):
            pick_ref[j] = jnp.where(obs_wide_ref[j] == k + 1, seen, pick_ref[j])
        return carry

    lax.fori_loop(0, steps, forward, 0)

    square = jnp.zeros((rows, seen_width), F32)
    for j in range(seen_count):
        misfit = pick_ref[j] - target_ref[pl.ds(j, rows, stride=seen_count), :]
        square = square + misfit * misfit
        pick_ref[j] = misfit.astype(BF16).astype(F32)
    loglik = -0.5 * jnp.sum(square.T, axis=0, keepdims=True)
    kl_half = kl_ref[:, :rows]
    for part in range(1, width // rows):
        kl_half = kl_half + kl_ref[:, part * rows : (part + 1) * rows]
    kl_row = 0.5 * jnp.sum(kl_half.T, axis=0, keepdims=True)
    divisor = (width * length_ref[...] + seen_width * seen_count).astype(F32)
    elbo_ref[...] = (loglik - kl_row) / divisor

    cot_ref[...] = jnp.zeros_like(cot_ref)

    def backward(index, carry):
        k = steps - 1 - index
        total = jnp.zeros((rows, seen_width), F32)
        for j in range(seen_count):
            total = total + jnp.where(obs_wide_ref[j] == k + 1, pick_ref[j], 0.0)
        high = total.astype(BF16)
        low = (total - high.astype(F32)).astype(BF16)
        miss_ref[pl.ds(k * rows, rows), :seen_width] = high
        miss_ref[pl.ds(k * rows, rows), seen_width:] = low
        obs_back = dot_nt(high, dec_ref[...]) + dot_nt(low, dec_ref[...])
        cot = cot_ref[...] + obs_back
        scaled = scaled_ref[k]
        factor = both(jnp.where(k < len_ref[...], dt_ref[...], 0.0))
        update = factor * (cot + scaled)
        rounded = update.astype(BF16)
        ut_ref[:, pl.ds(pl.multiple_of(k * rows, rows), rows)] = rounded.T
        sum_b_out_ref[...] += fold(update)
        cot = cot + factor * rate_ref[...] * scaled
        for n in range(chunks):
            act = act_ref[n, pl.ds(k * rows, rows), :].astype(F32)
            pre = dot_nt(rounded, w_out_ref[n]) * (1.0 - act * act)
            sum_b_in_ref[n] += fold(pre)
            pre_round = pre.astype(BF16)
            pre_ref[n, pl.ds(k * rows, rows), :] = pre_round
            cot = cot + dot_nt(pre_round, w_in_ref[n])
        cot_ref[...] = cot
        return carry

    lax.fori_loop(0, steps, backward, 0)

    def gradients(n, carry):
        grads_ref[n, :width, :] = dot(xt_ref[...], pre_ref[n])
        grads_ref[n, width : 2 * width, :] = dot(ut_ref[...], act_ref[n]).T
        return carry

    lax.fori_loop(0, chunks, gradients, 0)

    dec_grad = jnp.zeros((width, 2 * seen_width), F32)
    dec_grad = dec_grad + dot(xt_ref[:, rows:], miss_ref[: (steps - 1) * rows, :])
    last = lax.dot_general(
        x_ref[steps],
        miss_ref[(steps - 1) * rows :, :],
        (((0,), (0,)), ((), ())),
        preferred_element_type=F32,
    )
    dec_grad = dec_grad + last
    dec_grad = dec_grad[:, :seen_width] + dec_grad[:, seen_width:]
    lanes = width // seen_width
    share = width // chunks
    tail = 2 * width
    line = tail + share // lanes
    for n in range(chunks):
        pieces = [
            dec_grad[n * share + m * share // lanes : n * share + (m + 1) * share // lanes, :]
            for m in range(lanes)
        ]
        grads_ref[n, tail:line, :] = jnp.concatenate(pieces, axis=1)
        grads_ref[n, line:, :] = jnp.zeros((grads_ref.shape[1] - line, width), F32)
        grads_ref[n, line : line + 1, :] = jnp.sum(sum_b_in_ref[n], axis=0, keepdims=True)
        grads_ref[n, line + 1 : line + 2, :] = jnp.sum(
            sum_b_out_ref[...], axis=0, keepdims=True
        )
        grads_ref[n, line + 2 : line + 3, :rows] = loglik
        grads_ref[n, line + 2 : line + 3, rows : 2 * rows] = kl_row


def core(grad_rows, init, noise, step, length, obs, seen, w_in, b_in, w_out, b_out, dec, rate, diff):
    rows, width = init.shape
    steps = noise.shape[0]
    seen_count, seen_width = seen.shape[1], dec.shape[1]
    chunks = w_in.shape[0]
    vmem = pl.BlockSpec(memory_space=pltpu.VMEM)
    out = [
        jax.ShapeDtypeStruct((1, rows), F32),
        jax.ShapeDtypeStruct((chunks, grad_rows, width), F32),
        jax.ShapeDtypeStruct((rows, width), F32),
    ]
    scratch = [
        pltpu.VMEM((steps + 1, rows, width), BF16),
        pltpu.VMEM((width, steps * rows), BF16),
        pltpu.VMEM((width, steps * rows), BF16),
        pltpu.VMEM((chunks, steps * rows, width), BF16),
        pltpu.VMEM((chunks, steps * rows, width), BF16),
        pltpu.VMEM((steps, rows, width), F32),
        pltpu.VMEM((seen_count, rows, seen_width), F32),
        pltpu.VMEM((seen_count, rows, rows), jnp.int32),
        pltpu.VMEM((rows, rows), F32),
        pltpu.VMEM((rows, rows), F32),
        pltpu.VMEM((rows, rows), jnp.int32),
        pltpu.VMEM((rows, width), F32),
        pltpu.VMEM((rows, width), F32),
        pltpu.VMEM((chunks, 8, width), F32),
        pltpu.VMEM((8, width), F32),
        pltpu.VMEM((steps * rows, 2 * seen_width), BF16),
        pltpu.VMEM((rows * seen_count, seen_width), F32),
    ]
    return pl.pallas_call(
        core_kernel,
        out_shape=out,
        in_specs=[vmem] * 13,
        out_specs=[vmem] * 3,
        scratch_shapes=scratch,
        compiler_params=pltpu.CompilerParams(vmem_limit_bytes=44 * 1024 * 1024),
        cost_estimate=pl.CostEstimate(
            flops=12 * steps * rows * width * width * chunks,
            bytes_accessed=8 << 20,
            transcendentals=steps * rows * width * chunks,
        ),
        name="sde",
    )(init, noise, step, length, obs, seen, w_in, b_in, w_out, b_out, dec, rate, diff)


def send(source, target, send_sem, recv_sem, peer):
    return pltpu.make_async_remote_copy(
        src_ref=source,
        dst_ref=target,
        send_sem=send_sem,
        recv_sem=recv_sem,
        device_id=peer,
        device_id_type=pl.DeviceIdType.MESH,
    )


def greet(peers):
    barrier = pltpu.get_barrier_semaphore()
    for peer in peers:
        pl.semaphore_signal(barrier, inc=1, device_id=peer, device_id_type=pl.DeviceIdType.MESH)
    pl.semaphore_wait(barrier, len(peers))


def mp_places():
    mine = lax.axis_index("mp")
    chip, unit = mine // 2, mine % 2
    sibling = chip * 2 + (1 - unit)
    across = (1 - chip) * 2 + unit
    diagonal = (1 - chip) * 2 + (1 - unit)
    return mine, sibling, across, diagonal


def gather_kernel(w_in_ref, w_out_ref, b_in_ref, all_in_ref, all_out_ref, all_b_ref, bias_ref, send_sem, recv_sem):
    mine, sibling, across, diagonal = mp_places()
    batch = lax.axis_index("batch")
    to_across, to_sibling = (batch, across), (batch, sibling)
    bias_ref[...] = jnp.broadcast_to(b_in_ref[...].astype(F32), bias_ref.shape)
    greet([to_across, to_sibling])
    pairs = ((w_in_ref, all_in_ref), (w_out_ref, all_out_ref), (bias_ref, all_b_ref))
    far, near, relayed = [], [], []
    for i, (own, whole) in enumerate(pairs):
        copy = send(own, whole.at[mine], send_sem.at[0, i], recv_sem.at[0, i], to_across)
        copy.start()
        far.append(copy)
    for i, (own, whole) in enumerate(pairs):
        copy = send(own, whole.at[mine], send_sem.at[1, i], recv_sem.at[1, i], to_sibling)
        copy.start()
        near.append(copy)
    for own, whole in pairs:
        whole[mine] = own[...]
    for i, (own, whole) in enumerate(pairs):
        far[i].wait_recv()
        copy = send(
            whole.at[across], whole.at[across], send_sem.at[2, i], recv_sem.at[2, i], to_sibling
        )
        copy.start()
        relayed.append(copy)
    for copy in far:
        copy.wait_send()
    for copy in near + relayed:
        copy.wait()


def gather(w_in, w_out, b_in):
    count = lax.axis_size("mp")
    vmem = pl.BlockSpec(memory_space=pltpu.VMEM)
    return pl.pallas_call(
        gather_kernel,
        out_shape=[
            jax.ShapeDtypeStruct((count,) + w_in.shape, BF16),
            jax.ShapeDtypeStruct((count,) + w_out.shape, BF16),
            jax.ShapeDtypeStruct((count, 8, b_in.shape[1]), F32),
        ],
        in_specs=[vmem] * 3,
        out_specs=[vmem] * 3,
        scratch_shapes=[
            pltpu.VMEM((8, b_in.shape[1]), F32),
            pltpu.SemaphoreType.DMA((3, 3)),
            pltpu.SemaphoreType.DMA((3, 3)),
        ],
        compiler_params=pltpu.CompilerParams(
            collective_id=0, has_side_effects=True, vmem_limit_bytes=8 * 1024 * 1024
        ),
        cost_estimate=pl.CostEstimate(flops=0, bytes_accessed=32 << 20, transcendentals=0),
        name="gather_weights",
    )(w_in, w_out, b_in)


def reduce_kernel(
    members,
    total,
    share,
    grads_ref,
    w_in_ref,
    w_out_ref,
    b_in_ref,
    b_out_ref,
    dec_ref,
    scores_ref,
    near_ref,
    far_w_ref,
    far_t_ref,
    got_w_ref,
    got_t_ref,
    full_ref,
    round_ref,
    parts_ref,
    done_ref,
    decs_ref,
    near_send,
    near_recv,
    far_send,
    far_recv,
    rs_send,
    rs_recv,
    ag_send,
    ag_recv,
    dec_send,
    dec_recv,
):
    mine, sibling, across, diagonal = mp_places()
    batch = lax.axis_index("batch")
    width = grads_ref.shape[2]
    weight_rows = 2 * width
    piece = grads_ref.shape[1] // members
    others = [(lax.rem(batch + d, members), mine) for d in range(1, members)]
    group = [(batch, sibling), (batch, across), (batch, diagonal)]
    greet(group + others)
    near = []
    for i, quarter in enumerate((diagonal, sibling)):
        copy = send(
            grads_ref.at[quarter], near_ref.at[i], near_send.at[i], near_recv.at[i], group[0]
        )
        copy.start()
        near.append(copy)
    near[0].wait_recv()
    far_w_ref[...] = (
        grads_ref[across, :weight_rows, :] + near_ref[0, :weight_rows, :]
    ).astype(BF16)
    far_t_ref[...] = grads_ref[across, weight_rows:, :] + near_ref[0, weight_rows:, :]
    far = [
        send(far_w_ref, got_w_ref, far_send.at[0], far_recv.at[0], group[1]),
        send(far_t_ref, got_t_ref, far_send.at[1], far_recv.at[1], group[1]),
    ]
    for copy in far:
        copy.start()
    near[1].wait_recv()
    full_ref[...] = grads_ref[mine] + near_ref[1]
    far[0].wait_recv()
    full_ref[:weight_rows, :] += got_w_ref[...].astype(F32)
    far[1].wait_recv()
    full_ref[weight_rows:, :] += got_t_ref[...]
    for p in range(members):
        round_ref[p] = full_ref[p * piece : (p + 1) * piece, :].astype(BF16)
    scatter = []
    for d in range(1, members):
        target = lax.rem(batch + d, members)
        copy = send(
            round_ref.at[target],
            parts_ref.at[d - 1],
            rs_send.at[d - 1],
            rs_recv.at[d - 1],
            others[d - 1],
        )
        copy.start()
        scatter.append(copy)
    here = pl.ds(pl.multiple_of(batch * piece, 8), piece)
    value = full_ref[here, :]
    for d in range(1, members):
        scatter[d - 1].wait_recv()
        value = value + parts_ref[d - 1].astype(F32)
    done_ref[here, :] = value / total
    spread = []
    for d in range(1, members):
        copy = send(
            done_ref.at[here, :],
            done_ref.at[here, :],
            ag_send.at[d - 1],
            ag_recv.at[d - 1],
            others[d - 1],
        )
        copy.start()
        spread.append(copy)
    for copy in near + far + scatter:
        copy.wait_send()
    for d in range(1, members):
        origin = lax.rem(batch + members - d, members)
        there = pl.ds(pl.multiple_of(origin * piece, 8), piece)
        send(
            done_ref.at[there, :],
            done_ref.at[there, :],
            ag_send.at[d - 1],
            ag_recv.at[d - 1],
            others[d - 1],
        ).wait_recv()
    dec_rows = decs_ref.shape[1]
    line = weight_rows + dec_rows
    exchange = []
    for i in range(3):
        copy = send(
            done_ref.at[pl.ds(weight_rows, dec_rows), :],
            decs_ref.at[mine],
            dec_send.at[i],
            dec_recv.at[i],
            group[i],
        )
        copy.start()
        exchange.append(copy)
    w_in_ref[...] = done_ref[:width, :]
    w_out_ref[...] = done_ref[width:weight_rows, :]
    decs_ref[mine] = done_ref[weight_rows:line, :]
    b_in_ref[...] = done_ref[line : line + 1, :]
    b_out_ref[...] = done_ref[line + 1 : line + 2, :]
    half = share
    scores_ref[:, 0:1] = jnp.sum(done_ref[line + 2 : line + 3, :half], axis=1, keepdims=True)
    scores_ref[:, 1:2] = jnp.sum(
        done_ref[line + 2 : line + 3, half : 2 * half], axis=1, keepdims=True
    )
    for copy in spread:
        copy.wait_send()
    for i, origin in enumerate((sibling, across, diagonal)):
        exchange[i].wait_send()
        send(
            decs_ref.at[origin], decs_ref.at[origin], dec_send.at[i], dec_recv.at[i], group[i]
        ).wait_recv()
    seen_width = dec_ref.shape[1]
    for n in range(decs_ref.shape[0]):
        for m in range(width // seen_width):
            start = (n * (width // seen_width) + m) * dec_rows
            dec_ref[start : start + dec_rows, :] = decs_ref[
                n, :, m * seen_width : (m + 1) * seen_width
            ]


def reduce_all(grads, rows, seen_width):
    quarters, grad_rows, width = grads.shape
    members = lax.axis_size("batch")
    total = rows * members * lax.axis_size("mp")
    dec_rows = width // quarters // (width // seen_width)
    tail_rows = grad_rows - 2 * width
    piece = grad_rows // members
    vmem = pl.BlockSpec(memory_space=pltpu.VMEM)
    sems = []
    for count in (2, 2, members - 1, members - 1, 3):
        sems += [pltpu.SemaphoreType.DMA((count,))] * 2

    def body(*refs):
        reduce_kernel(members, total, rows, *refs)

    return pl.pallas_call(
        body,
        out_shape=[
            jax.ShapeDtypeStruct((width, width), F32),
            jax.ShapeDtypeStruct((width, width), F32),
            jax.ShapeDtypeStruct((1, width), F32),
            jax.ShapeDtypeStruct((1, width), F32),
            jax.ShapeDtypeStruct((width, seen_width), F32),
            jax.ShapeDtypeStruct((1, 2), F32),
        ],
        in_specs=[vmem],
        out_specs=[vmem] * 6,
        scratch_shapes=[
            pltpu.VMEM((2, grad_rows, width), F32),
            pltpu.VMEM((2 * width, width), BF16),
            pltpu.VMEM((tail_rows, width), F32),
            pltpu.VMEM((2 * width, width), BF16),
            pltpu.VMEM((tail_rows, width), F32),
            pltpu.VMEM((grad_rows, width), F32),
            pltpu.VMEM((members, piece, width), BF16),
            pltpu.VMEM((members - 1, piece, width), BF16),
            pltpu.VMEM((grad_rows, width), F32),
            pltpu.VMEM((quarters, dec_rows, width), F32),
        ]
        + sems,
        compiler_params=pltpu.CompilerParams(
            collective_id=1, has_side_effects=True, vmem_limit_bytes=16 * 1024 * 1024
        ),
        name="reduce_grads",
    )(grads)


def on_device(
    init_state,
    brownian,
    step_size,
    lengths,
    obs_steps,
    observed,
    w_in,
    b_in,
    w_out,
    b_out,
    decoder,
    prior_rate,
    diffusion,
):
    rows, width = init_state.shape
    seen_width = decoder.shape[1]
    w_in_all, w_out_all, b_in_all = gather(w_in, w_out, b_in[None, :])
    unit = 8 * lax.axis_size("batch")
    need = 2 * width + width // lax.axis_size("mp") * seen_width // width + 3
    elbo, grads, cot = core(
        -(-need // unit) * unit,
        init_state,
        brownian,
        step_size[None, :],
        lengths[None, :],
        obs_steps.T,
        observed,
        w_in_all,
        b_in_all,
        w_out_all,
        b_out[None, :],
        decoder,
        prior_rate[None, :],
        diffusion[None, :],
    )
    own_w_in, own_w_out, own_b_in, b_out_grad, dec_grad, scores = reduce_all(
        grads, rows, seen_width
    )
    return (
        elbo[0],
        scores[0],
        own_w_in,
        own_b_in[0],
        own_w_out,
        b_out_grad[0],
        dec_grad,
        cot,
    )


def solution(mesh):
    both = ("batch", "mp")
    placed = (
        P(both, None),
        P(None, both, None),
        P(both),
        P(both),
        P(both, None),
        P(both, None, None),
        P(None, "mp"),
        P("mp"),
        P("mp", None),
        P(),
        P(),
        P(),
        P(),
    )
    return jax.shard_map(
        on_device,
        mesh=mesh,
        in_specs=placed,
        out_specs=(
            P(both),
            P(),
            P(None, "mp"),
            P("mp"),
            P("mp", None),
            P(),
            P(),
            P(both, None),
        ),
        check_vma=False,
    )
```

```python
import jax
import jax.numpy as jnp
from jax import lax
from jax.experimental import pallas as pl
from jax.experimental.pallas import tpu as pltpu
from jax.sharding import PartitionSpec as P

F32 = jnp.float32
BF16 = jnp.bfloat16
NT = (((1,), (1,)), ((), ()))


def dot(a, b):
    return jnp.dot(a, b, preferred_element_type=F32)


def dot_nt(a, b):
    return lax.dot_general(a, b, NT, preferred_element_type=F32)


def fold(value):
    return value.reshape(-1, 8, value.shape[1]).sum(axis=0)


def core_kernel(
    init_ref,
    noise_ref,
    step_ref,
    length_ref,
    obs_ref,
    seen_ref,
    w_in_ref,
    b_in_ref,
    w_out_ref,
    b_out_ref,
    dec_ref,
    rate_ref,
    diff_ref,
    elbo_ref,
    grads_ref,
    cot_ref,
    x_ref,
    xt_ref,
    ut_ref,
    act_ref,
    pre_ref,
    scaled_ref,
    pick_ref,
    obs_wide_ref,
    dt_ref,
    root_ref,
    len_ref,
    state_ref,
    kl_ref,
    sum_b_in_ref,
    sum_b_out_ref,
    miss_ref,
    target_ref,
):
    rows, width = init_ref.shape
    steps = noise_ref.shape[0]
    seen_count = obs_ref.shape[0]
    seen_width = dec_ref.shape[1]
    chunks = w_in_ref.shape[0]

    def column(row):
        return jnp.broadcast_to(row, (rows, rows)).T

    dt_ref[...] = column(step_ref[...])
    root_ref[...] = jnp.sqrt(dt_ref[...])
    len_ref[...] = column(length_ref[...])
    for j in range(seen_count):
        obs_wide_ref[j] = column(obs_ref[j : j + 1, :])
    target_ref[...] = seen_ref[...].astype(F32).reshape(target_ref.shape)
    pick_ref[...] = jnp.zeros_like(pick_ref)
    kl_ref[...] = jnp.zeros_like(kl_ref)
    sum_b_in_ref[...] = jnp.zeros_like(sum_b_in_ref)
    sum_b_out_ref[...] = jnp.zeros_like(sum_b_out_ref)
    state_ref[...] = init_ref[...]
    x_ref[0] = init_ref[...].astype(BF16)

    def both(value):
        return jnp.concatenate([value] * (width // rows), axis=1)

    def forward(k, carry):
        x = x_ref[k]
        drift = jnp.broadcast_to(b_out_ref[...], (rows, width))
        for n in range(chunks):
            act = jnp.tanh(dot(x, w_in_ref[n]) + b_in_ref[n, :1, :]).astype(BF16)
            act_ref[n, pl.ds(k * rows, rows), :] = act
            drift = drift + dot(act, w_out_ref[n])
        state = state_ref[...]
        inv = 1.0 / diff_ref[...]
        live = k < len_ref[...]
        factor = both(jnp.where(live, dt_ref[...], 0.0))
        root = both(jnp.where(live, root_ref[...], 0.0))
        residual = (drift + rate_ref[...] * state) * inv
        kl_ref[...] += factor * residual * residual
        scaled_ref[k] = residual * inv
        following = state + (
            factor * drift + diff_ref[...] * root * noise_ref[k].astype(F32)
        )
        state_ref[...] = following
        rounded = following.astype(BF16)
        x_ref[k + 1] = rounded
        xt_ref[:, pl.ds(pl.multiple_of(k * rows, rows), rows)] = x.T
        seen = dot(rounded, dec_ref[...])
        for j in range(seen_count):
            pick_ref[j] = jnp.where(obs_wide_ref[j] == k + 1, seen, pick_ref[j])
        return carry

    lax.fori_loop(0, steps, forward, 0)

    square = jnp.zeros((rows, seen_width), F32)
    for j in range(seen_count):
        misfit = pick_ref[j] - target_ref[pl.ds(j, rows, stride=seen_count), :]
        square = square + misfit * misfit
        pick_ref[j] = misfit.astype(BF16).astype(F32)
    loglik = -0.5 * jnp.sum(square.T, axis=0, keepdims=True)
    kl_half = kl_ref[:, :rows]
    for part in range(1, width // rows):
        kl_half = kl_half + kl_ref[:, part * rows : (part + 1) * rows]
    kl_row = 0.5 * jnp.sum(kl_half.T, axis=0, keepdims=True)
    divisor = (width * length_ref[...] + seen_width * seen_count).astype(F32)
    elbo_ref[...] = (loglik - kl_row) / divisor

    cot_ref[...] = jnp.zeros_like(cot_ref)

    def backward(index, carry):
        k = steps - 1 - index
        total = jnp.zeros((rows, seen_width), F32)
        for j in range(seen_count):
            total = total + jnp.where(obs_wide_ref[j] == k + 1, pick_ref[j], 0.0)
        high = total.astype(BF16)
        low = (total - high.astype(F32)).astype(BF16)
        miss_ref[pl.ds(k * rows, rows), :seen_width] = high
        miss_ref[pl.ds(k * rows, rows), seen_width:] = low
        obs_back = dot_nt(high, dec_ref[...]) + dot_nt(low, dec_ref[...])
        cot = cot_ref[...] + obs_back
        scaled = scaled_ref[k]
        factor = both(jnp.where(k < len_ref[...], dt_ref[...], 0.0))
        update = factor * (cot + scaled)
        rounded = update.astype(BF16)
        ut_ref[:, pl.ds(pl.multiple_of(k * rows, rows), rows)] = rounded.T
        sum_b_out_ref[...] += fold(update)
        cot = cot + factor * rate_ref[...] * scaled
        for n in range(chunks):
            act = act_ref[n, pl.ds(k * rows, rows), :].astype(F32)
            pre = dot_nt(rounded, w_out_ref[n]) * (1.0 - act * act)
            sum_b_in_ref[n] += fold(pre)
            pre_round = pre.astype(BF16)
            pre_ref[n, pl.ds(k * rows, rows), :] = pre_round
            cot = cot + dot_nt(pre_round, w_in_ref[n])
        cot_ref[...] = cot
        return carry

    lax.fori_loop(0, steps, backward, 0)

    def gradients(n, carry):
        grads_ref[n, :width, :] = dot(xt_ref[...], pre_ref[n])
        grads_ref[n, width : 2 * width, :] = dot(ut_ref[...], act_ref[n]).T
        return carry

    lax.fori_loop(0, chunks, gradients, 0)

    dec_grad = jnp.zeros((width, 2 * seen_width), F32)
    dec_grad = dec_grad + dot(xt_ref[:, rows:], miss_ref[: (steps - 1) * rows, :])
    last = lax.dot_general(
        x_ref[steps],
        miss_ref[(steps - 1) * rows :, :],
        (((0,), (0,)), ((), ())),
        preferred_element_type=F32,
    )
    dec_grad = dec_grad + last
    dec_grad = dec_grad[:, :seen_width] + dec_grad[:, seen_width:]
    lanes = width // seen_width
    share = width // chunks
    tail = 2 * width
    line = tail + share // lanes
    for n in range(chunks):
        pieces = [
            dec_grad[n * share + m * share // lanes : n * share + (m + 1) * share // lanes, :]
            for m in range(lanes)
        ]
        grads_ref[n, tail:line, :] = jnp.concatenate(pieces, axis=1)
        grads_ref[n, line:, :] = jnp.zeros((grads_ref.shape[1] - line, width), F32)
        grads_ref[n, line : line + 1, :] = jnp.sum(sum_b_in_ref[n], axis=0, keepdims=True)
        grads_ref[n, line + 1 : line + 2, :] = jnp.sum(
            sum_b_out_ref[...], axis=0, keepdims=True
        )
        grads_ref[n, line + 2 : line + 3, :rows] = loglik
        grads_ref[n, line + 2 : line + 3, rows : 2 * rows] = kl_row


def core(grad_rows, init, noise, step, length, obs, seen, w_in, b_in, w_out, b_out, dec, rate, diff):
    rows, width = init.shape
    steps = noise.shape[0]
    seen_count, seen_width = seen.shape[1], dec.shape[1]
    chunks = w_in.shape[0]
    vmem = pl.BlockSpec(memory_space=pltpu.VMEM)
    out = [
        jax.ShapeDtypeStruct((1, rows), F32),
        jax.ShapeDtypeStruct((chunks, grad_rows, width), F32),
        jax.ShapeDtypeStruct((rows, width), F32),
    ]
    resident = (6, 7, 8)
    operands = (init, noise, step, length, obs, seen, w_in, b_in, w_out, b_out, dec, rate, diff)
    loaded = [i for i in range(len(operands)) if i not in resident]
    specs = [
        vmem if i in resident else pl.BlockSpec(memory_space=pltpu.HBM)
        for i in range(len(operands))
    ]

    def body(*refs):
        refs = list(refs)
        sems = refs.pop()
        spaces = [refs.pop() for _ in loaded][::-1]
        copies = []
        for at, (i, space) in enumerate(zip(loaded, spaces)):
            copy = pltpu.make_async_copy(refs[i], space, sems.at[at])
            copy.start()
            copies.append(copy)
            refs[i] = space
        for copy in copies:
            copy.wait()
        core_kernel(*refs)

    scratch = [
        pltpu.VMEM((steps + 1, rows, width), BF16),
        pltpu.VMEM((width, steps * rows), BF16),
        pltpu.VMEM((width, steps * rows), BF16),
        pltpu.VMEM((chunks, steps * rows, width), BF16),
        pltpu.VMEM((chunks, steps * rows, width), BF16),
        pltpu.VMEM((steps, rows, width), F32),
        pltpu.VMEM((seen_count, rows, seen_width), F32),
        pltpu.VMEM((seen_count, rows, rows), jnp.int32),
        pltpu.VMEM((rows, rows), F32),
        pltpu.VMEM((rows, rows), F32),
        pltpu.VMEM((rows, rows), jnp.int32),
        pltpu.VMEM((rows, width), F32),
        pltpu.VMEM((rows, width), F32),
        pltpu.VMEM((chunks, 8, width), F32),
        pltpu.VMEM((8, width), F32),
        pltpu.VMEM((steps * rows, 2 * seen_width), BF16),
        pltpu.VMEM((rows * seen_count, seen_width), F32),
    ]
    scratch += [pltpu.VMEM(operands[i].shape, operands[i].dtype) for i in loaded]
    scratch += [pltpu.SemaphoreType.DMA((len(loaded),))]
    return pl.pallas_call(
        body,
        out_shape=out,
        in_specs=specs,
        out_specs=[vmem] * 3,
        scratch_shapes=scratch,
        compiler_params=pltpu.CompilerParams(vmem_limit_bytes=60 * 1024 * 1024),
        cost_estimate=pl.CostEstimate(
            flops=12 * steps * rows * width * width * chunks,
            bytes_accessed=8 << 20,
            transcendentals=steps * rows * width * chunks,
        ),
        name="sde",
    )(*operands)


def send(source, target, send_sem, recv_sem, peer):
    return pltpu.make_async_remote_copy(
        src_ref=source,
        dst_ref=target,
        send_sem=send_sem,
        recv_sem=recv_sem,
        device_id=peer,
        device_id_type=pl.DeviceIdType.MESH,
    )


def greet(peers):
    barrier = pltpu.get_barrier_semaphore()
    for peer in peers:
        pl.semaphore_signal(barrier, inc=1, device_id=peer, device_id_type=pl.DeviceIdType.MESH)
    pl.semaphore_wait(barrier, len(peers))


def mp_places():
    mine = lax.axis_index("mp")
    chip, unit = mine // 2, mine % 2
    sibling = chip * 2 + (1 - unit)
    across = (1 - chip) * 2 + unit
    diagonal = (1 - chip) * 2 + (1 - unit)
    return mine, sibling, across, diagonal


def gather_kernel(w_in_ref, w_out_ref, b_in_ref, all_in_ref, all_out_ref, all_b_ref, bias_ref, send_sem, recv_sem):
    mine, sibling, across, diagonal = mp_places()
    batch = lax.axis_index("batch")
    to_across, to_sibling = (batch, across), (batch, sibling)
    bias_ref[...] = jnp.broadcast_to(b_in_ref[...].astype(F32), bias_ref.shape)
    greet([to_across, to_sibling])
    pairs = ((w_in_ref, all_in_ref), (w_out_ref, all_out_ref), (bias_ref, all_b_ref))
    far, near, relayed = [], [], []
    for i, (own, whole) in enumerate(pairs):
        copy = send(own, whole.at[mine], send_sem.at[0, i], recv_sem.at[0, i], to_across)
        copy.start()
        far.append(copy)
    for i, (own, whole) in enumerate(pairs):
        copy = send(own, whole.at[mine], send_sem.at[1, i], recv_sem.at[1, i], to_sibling)
        copy.start()
        near.append(copy)
    for own, whole in pairs:
        whole[mine] = own[...]
    for i, (own, whole) in enumerate(pairs):
        far[i].wait_recv()
        copy = send(
            whole.at[across], whole.at[across], send_sem.at[2, i], recv_sem.at[2, i], to_sibling
        )
        copy.start()
        relayed.append(copy)
    for copy in far:
        copy.wait_send()
    for copy in near + relayed:
        copy.wait()


def gather(w_in, w_out, b_in):
    count = lax.axis_size("mp")
    vmem = pl.BlockSpec(memory_space=pltpu.VMEM)
    return pl.pallas_call(
        gather_kernel,
        out_shape=[
            jax.ShapeDtypeStruct((count,) + w_in.shape, BF16),
            jax.ShapeDtypeStruct((count,) + w_out.shape, BF16),
            jax.ShapeDtypeStruct((count, 8, b_in.shape[1]), F32),
        ],
        in_specs=[vmem] * 3,
        out_specs=[vmem] * 3,
        scratch_shapes=[
            pltpu.VMEM((8, b_in.shape[1]), F32),
            pltpu.SemaphoreType.DMA((3, 3)),
            pltpu.SemaphoreType.DMA((3, 3)),
        ],
        compiler_params=pltpu.CompilerParams(
            collective_id=0, has_side_effects=True, vmem_limit_bytes=8 * 1024 * 1024
        ),
        cost_estimate=pl.CostEstimate(flops=0, bytes_accessed=32 << 20, transcendentals=0),
        name="gather_weights",
    )(w_in, w_out, b_in)


def reduce_kernel(
    members,
    total,
    grads_ref,
    done_ref,
    decs_ref,
    near_ref,
    far_w_ref,
    far_t_ref,
    got_w_ref,
    got_t_ref,
    full_ref,
    round_ref,
    parts_ref,
    near_send,
    near_recv,
    far_send,
    far_recv,
    rs_send,
    rs_recv,
    ag_send,
    ag_recv,
    pair_send,
    pair_recv,
    dec_send,
    dec_recv,
):
    mine, sibling, across, diagonal = mp_places()
    batch = lax.axis_index("batch")
    width = grads_ref.shape[2]
    weight_rows = 2 * width
    piece = grads_ref.shape[1] // members
    others = [(lax.rem(batch + d, members), mine) for d in range(1, members)]
    group = [(batch, sibling), (batch, across), (batch, diagonal)]
    greet(group + others)
    near = []
    for i, quarter in enumerate((diagonal, sibling)):
        copy = send(
            grads_ref.at[quarter], near_ref.at[i], near_send.at[i], near_recv.at[i], group[0]
        )
        copy.start()
        near.append(copy)
    near[0].wait_recv()
    far_w_ref[...] = (
        grads_ref[across, :weight_rows, :] + near_ref[0, :weight_rows, :]
    ).astype(BF16)
    far_t_ref[...] = grads_ref[across, weight_rows:, :] + near_ref[0, weight_rows:, :]
    far = [
        send(far_w_ref, got_w_ref, far_send.at[0], far_recv.at[0], group[1]),
        send(far_t_ref, got_t_ref, far_send.at[1], far_recv.at[1], group[1]),
    ]
    for copy in far:
        copy.start()
    near[1].wait_recv()
    full_ref[...] = grads_ref[mine] + near_ref[1]
    far[0].wait_recv()
    full_ref[:weight_rows, :] += got_w_ref[...].astype(F32)
    far[1].wait_recv()
    full_ref[weight_rows:, :] += got_t_ref[...]
    for p in range(members):
        round_ref[p] = full_ref[p * piece : (p + 1) * piece, :].astype(BF16)
    scatter = []
    for d in range(1, members):
        target = lax.rem(batch + d, members)
        copy = send(
            round_ref.at[target],
            parts_ref.at[d - 1],
            rs_send.at[d - 1],
            rs_recv.at[d - 1],
            others[d - 1],
        )
        copy.start()
        scatter.append(copy)
    here = pl.ds(pl.multiple_of(batch * piece, 8), piece)
    value = full_ref[here, :]
    for d in range(1, members):
        scatter[d - 1].wait_recv()
        value = value + parts_ref[d - 1].astype(F32)
    done_ref[here, :] = value / total
    pair = batch + 1 - 2 * (batch % 2)
    partner = (pair, mine)

    def rows_of(owner):
        return done_ref.at[pl.ds(pl.multiple_of(owner * piece, 8), piece), :]

    def relay(i, owner):
        return send(rows_of(owner), rows_of(owner), pair_send.at[i], pair_recv.at[i], partner)

    hops = members // 2
    spread = []
    for d in range(1, hops):
        target = lax.rem(batch + 2 * d, members)
        copy = send(
            rows_of(batch), rows_of(batch), ag_send.at[d - 1], ag_recv.at[d - 1], (target, mine)
        )
        copy.start()
        spread.append(copy)
    passed = [relay(0, batch)]
    passed[0].start()
    for copy in near + far + scatter:
        copy.wait_send()
    for d in range(1, hops):
        origin = lax.rem(batch + members - 2 * d, members)
        send(
            rows_of(origin),
            rows_of(origin),
            ag_send.at[d - 1],
            ag_recv.at[d - 1],
            (origin, mine),
        ).wait_recv()
        copy = relay(d, origin)
        copy.start()
        passed.append(copy)
    for d in range(hops):
        relay(d, lax.rem(pair + members - 2 * d, members)).wait_recv()
    spread += passed
    dec_rows = decs_ref.shape[1]
    exchange = []
    for i in range(3):
        copy = send(
            done_ref.at[pl.ds(weight_rows, dec_rows), :],
            decs_ref.at[mine],
            dec_send.at[i],
            dec_recv.at[i],
            group[i],
        )
        copy.start()
        exchange.append(copy)
    decs_ref[mine] = done_ref[weight_rows : weight_rows + dec_rows, :]
    for copy in spread:
        copy.wait_send()
    for i, origin in enumerate((sibling, across, diagonal)):
        exchange[i].wait_send()
        send(
            decs_ref.at[origin], decs_ref.at[origin], dec_send.at[i], dec_recv.at[i], group[i]
        ).wait_recv()


def finish_kernel(
    half, done_ref, decs_ref, w_in_ref, w_out_ref, b_in_ref, b_out_ref, dec_ref, scores_ref
):
    width = done_ref.shape[1]
    weight_rows = 2 * width
    dec_rows = decs_ref.shape[1]
    line = weight_rows + dec_rows
    w_in_ref[...] = done_ref[:width, :]
    w_out_ref[...] = done_ref[width:weight_rows, :]
    b_in_ref[...] = done_ref[line : line + 1, :]
    b_out_ref[...] = done_ref[line + 1 : line + 2, :]
    scores_ref[:, 0:1] = jnp.sum(done_ref[line + 2 : line + 3, :half], axis=1, keepdims=True)
    scores_ref[:, 1:2] = jnp.sum(
        done_ref[line + 2 : line + 3, half : 2 * half], axis=1, keepdims=True
    )
    seen_width = dec_ref.shape[1]
    for n in range(decs_ref.shape[0]):
        for m in range(width // seen_width):
            start = (n * (width // seen_width) + m) * dec_rows
            dec_ref[start : start + dec_rows, :] = decs_ref[
                n, :, m * seen_width : (m + 1) * seen_width
            ]


def reduce_all(grads, rows, seen_width):
    quarters, grad_rows, width = grads.shape
    members = lax.axis_size("batch")
    total = rows * members * lax.axis_size("mp")
    dec_rows = width // quarters // (width // seen_width)
    tail_rows = grad_rows - 2 * width
    piece = grad_rows // members
    vmem = pl.BlockSpec(memory_space=pltpu.VMEM)
    sems = []
    for count in (2, 2, members - 1, members // 2, members // 2, 3):
        sems += [pltpu.SemaphoreType.DMA((count,))] * 2

    def body(*refs):
        reduce_kernel(members, total, *refs)

    done, decs = pl.pallas_call(
        body,
        out_shape=[
            jax.ShapeDtypeStruct((grad_rows, width), F32),
            jax.ShapeDtypeStruct((quarters, dec_rows, width), F32),
        ],
        in_specs=[vmem],
        out_specs=[vmem] * 2,
        scratch_shapes=[
            pltpu.VMEM((2, grad_rows, width), F32),
            pltpu.VMEM((2 * width, width), BF16),
            pltpu.VMEM((tail_rows, width), F32),
            pltpu.VMEM((2 * width, width), BF16),
            pltpu.VMEM((tail_rows, width), F32),
            pltpu.VMEM((grad_rows, width), F32),
            pltpu.VMEM((members, piece, width), BF16),
            pltpu.VMEM((members - 1, piece, width), BF16),
        ]
        + sems,
        compiler_params=pltpu.CompilerParams(
            collective_id=1, has_side_effects=True, vmem_limit_bytes=16 * 1024 * 1024
        ),
        name="reduce_grads",
    )(grads)

    def finish(*refs):
        finish_kernel(rows, *refs)

    return pl.pallas_call(
        finish,
        out_shape=[
            jax.ShapeDtypeStruct((width, width), F32),
            jax.ShapeDtypeStruct((width, width), F32),
            jax.ShapeDtypeStruct((1, width), F32),
            jax.ShapeDtypeStruct((1, width), F32),
            jax.ShapeDtypeStruct((width, seen_width), F32),
            jax.ShapeDtypeStruct((1, 2), F32),
        ],
        in_specs=[vmem] * 2,
        out_specs=[vmem] * 6,
        compiler_params=pltpu.CompilerParams(vmem_limit_bytes=8 * 1024 * 1024),
        name="finish",
    )(done, decs)


def on_device(
    init_state,
    brownian,
    step_size,
    lengths,
    obs_steps,
    observed,
    w_in,
    b_in,
    w_out,
    b_out,
    decoder,
    prior_rate,
    diffusion,
):
    rows, width = init_state.shape
    seen_width = decoder.shape[1]
    w_in_all, w_out_all, b_in_all = gather(w_in, w_out, b_in[None, :])
    unit = 8 * lax.axis_size("batch")
    need = 2 * width + width // lax.axis_size("mp") * seen_width // width + 3
    elbo, grads, cot = core(
        -(-need // unit) * unit,
        init_state,
        brownian,
        step_size[None, :],
        lengths[None, :],
        obs_steps.T,
        observed,
        w_in_all,
        b_in_all,
        w_out_all,
        b_out[None, :],
        decoder,
        prior_rate[None, :],
        diffusion[None, :],
    )
    own_w_in, own_w_out, own_b_in, b_out_grad, dec_grad, scores = reduce_all(
        grads, rows, seen_width
    )
    return (
        elbo[0],
        scores[0],
        own_w_in,
        own_b_in[0],
        own_w_out,
        b_out_grad[0],
        dec_grad,
        cot,
    )


def solution(mesh):
    both = ("batch", "mp")
    placed = (
        P(both, None),
        P(None, both, None),
        P(both),
        P(both),
        P(both, None),
        P(both, None, None),
        P(None, "mp"),
        P("mp"),
        P("mp", None),
        P(),
        P(),
        P(),
        P(),
    )
    return jax.shard_map(
        on_device,
        mesh=mesh,
        in_specs=placed,
        out_specs=(
            P(both),
            P(),
            P(None, "mp"),
            P("mp"),
            P("mp", None),
            P(),
            P(),
            P(both, None),
        ),
        check_vma=False,
    )
```

```python
import jax
import jax.numpy as jnp
from jax import lax
from jax.experimental import pallas as pl
from jax.experimental.pallas import tpu as pltpu
from jax.sharding import PartitionSpec as P

F32 = jnp.float32
BF16 = jnp.bfloat16
NT = (((1,), (1,)), ((), ()))


def dot(a, b):
    return jnp.dot(a, b, preferred_element_type=F32)


def dot_nt(a, b):
    return lax.dot_general(a, b, NT, preferred_element_type=F32)


def fold(value):
    return value.reshape(-1, 8, value.shape[1]).sum(axis=0)


def core_kernel(
    init_ref,
    noise_ref,
    step_ref,
    length_ref,
    obs_ref,
    seen_ref,
    w_in_ref,
    b_in_ref,
    w_out_ref,
    b_out_ref,
    dec_ref,
    rate_ref,
    diff_ref,
    elbo_ref,
    grads_ref,
    cot_ref,
    x_ref,
    xt_ref,
    ut_ref,
    act_ref,
    pre_ref,
    scaled_ref,
    pick_ref,
    obs_wide_ref,
    dt_ref,
    root_ref,
    len_ref,
    state_ref,
    kl_ref,
    sum_b_in_ref,
    sum_b_out_ref,
    miss_ref,
    target_ref,
):
    rows, width = init_ref.shape
    steps = noise_ref.shape[0]
    seen_count = obs_ref.shape[0]
    seen_width = dec_ref.shape[1]
    chunks = w_in_ref.shape[0]

    def column(row):
        return jnp.broadcast_to(row, (rows, rows)).T

    dt_ref[...] = column(step_ref[...])
    root_ref[...] = jnp.sqrt(dt_ref[...])
    len_ref[...] = column(length_ref[...])
    for j in range(seen_count):
        obs_wide_ref[j] = column(obs_ref[j : j + 1, :])
    target_ref[...] = seen_ref[...].astype(F32).reshape(target_ref.shape)
    pick_ref[...] = jnp.zeros_like(pick_ref)
    kl_ref[...] = jnp.zeros_like(kl_ref)
    sum_b_in_ref[...] = jnp.zeros_like(sum_b_in_ref)
    sum_b_out_ref[...] = jnp.zeros_like(sum_b_out_ref)
    state_ref[...] = init_ref[...]
    x_ref[0] = init_ref[...].astype(BF16)

    def both(value):
        return jnp.concatenate([value] * (width // rows), axis=1)

    def forward(k, carry):
        x = x_ref[k]
        drift = jnp.broadcast_to(b_out_ref[...], (rows, width))
        for n in range(chunks):
            act = jnp.tanh(dot(x, w_in_ref[n]) + b_in_ref[n, :1, :]).astype(BF16)
            act_ref[n, pl.ds(k * rows, rows), :] = act
            drift = drift + dot(act, w_out_ref[n])
        state = state_ref[...]
        inv = 1.0 / diff_ref[...]
        live = k < len_ref[...]
        factor = both(jnp.where(live, dt_ref[...], 0.0))
        root = both(jnp.where(live, root_ref[...], 0.0))
        residual = (drift + rate_ref[...] * state) * inv
        kl_ref[...] += factor * residual * residual
        scaled_ref[k] = residual * inv
        following = state + (
            factor * drift + diff_ref[...] * root * noise_ref[k].astype(F32)
        )
        state_ref[...] = following
        rounded = following.astype(BF16)
        x_ref[k + 1] = rounded
        xt_ref[:, pl.ds(pl.multiple_of(k * rows, rows), rows)] = x.T
        seen = dot(rounded, dec_ref[...])
        for j in range(seen_count):
            pick_ref[j] = jnp.where(obs_wide_ref[j] == k + 1, seen, pick_ref[j])
        return carry

    lax.fori_loop(0, steps, forward, 0)

    square = jnp.zeros((rows, seen_width), F32)
    for j in range(seen_count):
        misfit = pick_ref[j] - target_ref[pl.ds(j, rows, stride=seen_count), :]
        square = square + misfit * misfit
        pick_ref[j] = misfit.astype(BF16).astype(F32)
    loglik = -0.5 * jnp.sum(square.T, axis=0, keepdims=True)
    kl_half = kl_ref[:, :rows]
    for part in range(1, width // rows):
        kl_half = kl_half + kl_ref[:, part * rows : (part + 1) * rows]
    kl_row = 0.5 * jnp.sum(kl_half.T, axis=0, keepdims=True)
    divisor = (width * length_ref[...] + seen_width * seen_count).astype(F32)
    elbo_ref[...] = (loglik - kl_row) / divisor

    cot_ref[...] = jnp.zeros_like(cot_ref)

    def backward(index, carry):
        k = steps - 1 - index
        total = jnp.zeros((rows, seen_width), F32)
        for j in range(seen_count):
            total = total + jnp.where(obs_wide_ref[j] == k + 1, pick_ref[j], 0.0)
        high = total.astype(BF16)
        low = (total - high.astype(F32)).astype(BF16)
        miss_ref[pl.ds(k * rows, rows), :seen_width] = high
        miss_ref[pl.ds(k * rows, rows), seen_width:] = low
        obs_back = dot_nt(
            jnp.concatenate([high, low], axis=1),
            jnp.concatenate([dec_ref[...], dec_ref[...]], axis=1),
        )
        cot = cot_ref[...] + obs_back
        scaled = scaled_ref[k]
        factor = both(jnp.where(k < len_ref[...], dt_ref[...], 0.0))
        update = factor * (cot + scaled)
        rounded = update.astype(BF16)
        ut_ref[:, pl.ds(pl.multiple_of(k * rows, rows), rows)] = rounded.T
        sum_b_out_ref[...] += fold(update)
        cot = cot + factor * rate_ref[...] * scaled
        for n in range(chunks):
            act = act_ref[n, pl.ds(k * rows, rows), :].astype(F32)
            pre = dot_nt(rounded, w_out_ref[n]) * (1.0 - act * act)
            sum_b_in_ref[n] += fold(pre)
            pre_round = pre.astype(BF16)
            pre_ref[n, pl.ds(k * rows, rows), :] = pre_round
            cot = cot + dot_nt(pre_round, w_in_ref[n])
        cot_ref[...] = cot
        return carry

    lax.fori_loop(0, steps, backward, 0)

    def gradients(n, carry):
        grads_ref[n, :width, :] = dot(xt_ref[...], pre_ref[n])
        grads_ref[n, width : 2 * width, :] = dot(ut_ref[...], act_ref[n]).T
        return carry

    lax.fori_loop(0, chunks, gradients, 0)

    dec_grad = jnp.zeros((width, 2 * seen_width), F32)
    dec_grad = dec_grad + dot(xt_ref[:, rows:], miss_ref[: (steps - 1) * rows, :])
    last = lax.dot_general(
        x_ref[steps],
        miss_ref[(steps - 1) * rows :, :],
        (((0,), (0,)), ((), ())),
        preferred_element_type=F32,
    )
    dec_grad = dec_grad + last
    dec_grad = dec_grad[:, :seen_width] + dec_grad[:, seen_width:]
    lanes = width // seen_width
    share = width // chunks
    tail = 2 * width
    line = tail + share // lanes
    for n in range(chunks):
        pieces = [
            dec_grad[n * share + m * share // lanes : n * share + (m + 1) * share // lanes, :]
            for m in range(lanes)
        ]
        grads_ref[n, tail:line, :] = jnp.concatenate(pieces, axis=1)
        grads_ref[n, line:, :] = jnp.zeros((grads_ref.shape[1] - line, width), F32)
        grads_ref[n, line : line + 1, :] = jnp.sum(sum_b_in_ref[n], axis=0, keepdims=True)
        grads_ref[n, line + 1 : line + 2, :] = jnp.sum(
            sum_b_out_ref[...], axis=0, keepdims=True
        )
        grads_ref[n, line + 2 : line + 3, :rows] = loglik
        grads_ref[n, line + 2 : line + 3, rows : 2 * rows] = kl_row


def core(grad_rows, init, noise, step, length, obs, seen, w_in, b_in, w_out, b_out, dec, rate, diff):
    rows, width = init.shape
    steps = noise.shape[0]
    seen_count, seen_width = seen.shape[1], dec.shape[1]
    chunks = w_in.shape[0]
    vmem = pl.BlockSpec(memory_space=pltpu.VMEM)
    out = [
        jax.ShapeDtypeStruct((1, rows), F32),
        jax.ShapeDtypeStruct((chunks, grad_rows, width), F32),
        jax.ShapeDtypeStruct((rows, width), F32),
    ]
    resident = (6, 7, 8)
    operands = (init, noise, step, length, obs, seen, w_in, b_in, w_out, b_out, dec, rate, diff)
    loaded = [i for i in range(len(operands)) if i not in resident]
    specs = [
        vmem if i in resident else pl.BlockSpec(memory_space=pltpu.HBM)
        for i in range(len(operands))
    ]

    def body(*refs):
        refs = list(refs)
        sems = refs.pop()
        spaces = [refs.pop() for _ in loaded][::-1]
        copies = []
        for at, (i, space) in enumerate(zip(loaded, spaces)):
            copy = pltpu.make_async_copy(refs[i], space, sems.at[at])
            copy.start()
            copies.append(copy)
            refs[i] = space
        for copy in copies:
            copy.wait()
        core_kernel(*refs)

    scratch = [
        pltpu.VMEM((steps + 1, rows, width), BF16),
        pltpu.VMEM((width, steps * rows), BF16),
        pltpu.VMEM((width, steps * rows), BF16),
        pltpu.VMEM((chunks, steps * rows, width), BF16),
        pltpu.VMEM((chunks, steps * rows, width), BF16),
        pltpu.VMEM((steps, rows, width), F32),
        pltpu.VMEM((seen_count, rows, seen_width), F32),
        pltpu.VMEM((seen_count, rows, rows), jnp.int32),
        pltpu.VMEM((rows, rows), F32),
        pltpu.VMEM((rows, rows), F32),
        pltpu.VMEM((rows, rows), jnp.int32),
        pltpu.VMEM((rows, width), F32),
        pltpu.VMEM((rows, width), F32),
        pltpu.VMEM((chunks, 8, width), F32),
        pltpu.VMEM((8, width), F32),
        pltpu.VMEM((steps * rows, 2 * seen_width), BF16),
        pltpu.VMEM((rows * seen_count, seen_width), F32),
    ]
    scratch += [pltpu.VMEM(operands[i].shape, operands[i].dtype) for i in loaded]
    scratch += [pltpu.SemaphoreType.DMA((len(loaded),))]
    return pl.pallas_call(
        body,
        out_shape=out,
        in_specs=specs,
        out_specs=[vmem] * 3,
        scratch_shapes=scratch,
        compiler_params=pltpu.CompilerParams(vmem_limit_bytes=60 * 1024 * 1024),
        cost_estimate=pl.CostEstimate(
            flops=12 * steps * rows * width * width * chunks,
            bytes_accessed=8 << 20,
            transcendentals=steps * rows * width * chunks,
        ),
        name="sde",
    )(*operands)


def send(source, target, send_sem, recv_sem, peer):
    return pltpu.make_async_remote_copy(
        src_ref=source,
        dst_ref=target,
        send_sem=send_sem,
        recv_sem=recv_sem,
        device_id=peer,
        device_id_type=pl.DeviceIdType.MESH,
    )


def greet(peers):
    barrier = pltpu.get_barrier_semaphore()
    for peer in peers:
        pl.semaphore_signal(barrier, inc=1, device_id=peer, device_id_type=pl.DeviceIdType.MESH)
    pl.semaphore_wait(barrier, len(peers))


def mp_places():
    mine = lax.axis_index("mp")
    chip, unit = mine // 2, mine % 2
    sibling = chip * 2 + (1 - unit)
    across = (1 - chip) * 2 + unit
    diagonal = (1 - chip) * 2 + (1 - unit)
    return mine, sibling, across, diagonal


def gather_kernel(w_in_ref, w_out_ref, b_in_ref, all_in_ref, all_out_ref, all_b_ref, bias_ref, send_sem, recv_sem):
    mine, sibling, across, diagonal = mp_places()
    batch = lax.axis_index("batch")
    to_across, to_sibling = (batch, across), (batch, sibling)
    bias_ref[...] = jnp.broadcast_to(b_in_ref[...].astype(F32), bias_ref.shape)
    greet([to_across, to_sibling])
    pairs = ((w_in_ref, all_in_ref), (w_out_ref, all_out_ref), (bias_ref, all_b_ref))
    far, near, relayed = [], [], []
    for i, (own, whole) in enumerate(pairs):
        copy = send(own, whole.at[mine], send_sem.at[0, i], recv_sem.at[0, i], to_across)
        copy.start()
        far.append(copy)
    for i, (own, whole) in enumerate(pairs):
        copy = send(own, whole.at[mine], send_sem.at[1, i], recv_sem.at[1, i], to_sibling)
        copy.start()
        near.append(copy)
    for own, whole in pairs:
        whole[mine] = own[...]
    for i, (own, whole) in enumerate(pairs):
        far[i].wait_recv()
        copy = send(
            whole.at[across], whole.at[across], send_sem.at[2, i], recv_sem.at[2, i], to_sibling
        )
        copy.start()
        relayed.append(copy)
    for copy in far:
        copy.wait_send()
    for copy in near + relayed:
        copy.wait()


def gather(w_in, w_out, b_in):
    count = lax.axis_size("mp")
    vmem = pl.BlockSpec(memory_space=pltpu.VMEM)
    return pl.pallas_call(
        gather_kernel,
        out_shape=[
            jax.ShapeDtypeStruct((count,) + w_in.shape, BF16),
            jax.ShapeDtypeStruct((count,) + w_out.shape, BF16),
            jax.ShapeDtypeStruct((count, 8, b_in.shape[1]), F32),
        ],
        in_specs=[vmem] * 3,
        out_specs=[vmem] * 3,
        scratch_shapes=[
            pltpu.VMEM((8, b_in.shape[1]), F32),
            pltpu.SemaphoreType.DMA((3, 3)),
            pltpu.SemaphoreType.DMA((3, 3)),
        ],
        compiler_params=pltpu.CompilerParams(
            collective_id=0, has_side_effects=True, vmem_limit_bytes=60 * 1024 * 1024
        ),
        cost_estimate=pl.CostEstimate(flops=0, bytes_accessed=32 << 20, transcendentals=0),
        name="gather_weights",
    )(w_in, w_out, b_in)


def reduce_kernel(
    members,
    total,
    grads_ref,
    done_ref,
    decs_ref,
    near_ref,
    far_w_ref,
    far_t_ref,
    got_w_ref,
    got_t_ref,
    full_ref,
    round_ref,
    parts_ref,
    near_send,
    near_recv,
    far_send,
    far_recv,
    rs_send,
    rs_recv,
    ag_send,
    ag_recv,
    pair_send,
    pair_recv,
    dec_send,
    dec_recv,
):
    mine, sibling, across, diagonal = mp_places()
    batch = lax.axis_index("batch")
    width = grads_ref.shape[2]
    weight_rows = 2 * width
    piece = grads_ref.shape[1] // members
    others = [(lax.rem(batch + d, members), mine) for d in range(1, members)]
    group = [(batch, sibling), (batch, across), (batch, diagonal)]
    greet(group + others)
    near = []
    for i, quarter in enumerate((diagonal, sibling)):
        copy = send(
            grads_ref.at[quarter], near_ref.at[i], near_send.at[i], near_recv.at[i], group[0]
        )
        copy.start()
        near.append(copy)
    near[0].wait_recv()
    far_w_ref[...] = (
        grads_ref[across, :weight_rows, :] + near_ref[0, :weight_rows, :]
    ).astype(BF16)
    far_t_ref[...] = grads_ref[across, weight_rows:, :] + near_ref[0, weight_rows:, :]
    far = [
        send(far_w_ref, got_w_ref, far_send.at[0], far_recv.at[0], group[1]),
        send(far_t_ref, got_t_ref, far_send.at[1], far_recv.at[1], group[1]),
    ]
    for copy in far:
        copy.start()
    near[1].wait_recv()
    full_ref[...] = grads_ref[mine] + near_ref[1]
    far[0].wait_recv()
    full_ref[:weight_rows, :] += got_w_ref[...].astype(F32)
    far[1].wait_recv()
    full_ref[weight_rows:, :] += got_t_ref[...]
    for p in range(members):
        round_ref[p] = full_ref[p * piece : (p + 1) * piece, :].astype(BF16)
    scatter = []
    for d in range(1, members):
        target = lax.rem(batch + d, members)
        copy = send(
            round_ref.at[target],
            parts_ref.at[d - 1],
            rs_send.at[d - 1],
            rs_recv.at[d - 1],
            others[d - 1],
        )
        copy.start()
        scatter.append(copy)
    here = pl.ds(pl.multiple_of(batch * piece, 8), piece)
    value = full_ref[here, :]
    for d in range(1, members):
        scatter[d - 1].wait_recv()
        value = value + parts_ref[d - 1].astype(F32)
    done_ref[here, :] = value / total
    pair = batch + 1 - 2 * (batch % 2)
    partner = (pair, mine)

    def rows_of(owner):
        return done_ref.at[pl.ds(pl.multiple_of(owner * piece, 8), piece), :]

    def relay(i, owner):
        return send(rows_of(owner), rows_of(owner), pair_send.at[i], pair_recv.at[i], partner)

    hops = members // 2
    spread = []
    for d in range(1, hops):
        target = lax.rem(batch + 2 * d, members)
        copy = send(
            rows_of(batch), rows_of(batch), ag_send.at[d - 1], ag_recv.at[d - 1], (target, mine)
        )
        copy.start()
        spread.append(copy)
    passed = [relay(0, batch)]
    passed[0].start()
    for copy in near + far + scatter:
        copy.wait_send()
    for d in range(1, hops):
        origin = lax.rem(batch + members - 2 * d, members)
        send(
            rows_of(origin),
            rows_of(origin),
            ag_send.at[d - 1],
            ag_recv.at[d - 1],
            (origin, mine),
        ).wait_recv()
        copy = relay(d, origin)
        copy.start()
        passed.append(copy)
    for d in range(hops):
        relay(d, lax.rem(pair + members - 2 * d, members)).wait_recv()
    spread += passed
    dec_rows = decs_ref.shape[1]
    exchange = []
    for i in range(3):
        copy = send(
            done_ref.at[pl.ds(weight_rows, dec_rows), :],
            decs_ref.at[mine],
            dec_send.at[i],
            dec_recv.at[i],
            group[i],
        )
        copy.start()
        exchange.append(copy)
    decs_ref[mine] = done_ref[weight_rows : weight_rows + dec_rows, :]
    for copy in spread:
        copy.wait_send()
    for i, origin in enumerate((sibling, across, diagonal)):
        exchange[i].wait_send()
        send(
            decs_ref.at[origin], decs_ref.at[origin], dec_send.at[i], dec_recv.at[i], group[i]
        ).wait_recv()


def finish_kernel(
    half, done_ref, decs_ref, w_in_ref, w_out_ref, b_in_ref, b_out_ref, dec_ref, scores_ref
):
    width = done_ref.shape[1]
    weight_rows = 2 * width
    dec_rows = decs_ref.shape[1]
    line = weight_rows + dec_rows
    w_in_ref[...] = done_ref[:width, :]
    w_out_ref[...] = done_ref[width:weight_rows, :]
    b_in_ref[...] = done_ref[line : line + 1, :]
    b_out_ref[...] = done_ref[line + 1 : line + 2, :]
    scores_ref[:, 0:1] = jnp.sum(done_ref[line + 2 : line + 3, :half], axis=1, keepdims=True)
    scores_ref[:, 1:2] = jnp.sum(
        done_ref[line + 2 : line + 3, half : 2 * half], axis=1, keepdims=True
    )
    seen_width = dec_ref.shape[1]
    for n in range(decs_ref.shape[0]):
        for m in range(width // seen_width):
            start = (n * (width // seen_width) + m) * dec_rows
            dec_ref[start : start + dec_rows, :] = decs_ref[
                n, :, m * seen_width : (m + 1) * seen_width
            ]


def reduce_all(grads, rows, seen_width):
    quarters, grad_rows, width = grads.shape
    members = lax.axis_size("batch")
    total = rows * members * lax.axis_size("mp")
    dec_rows = width // quarters // (width // seen_width)
    tail_rows = grad_rows - 2 * width
    piece = grad_rows // members
    vmem = pl.BlockSpec(memory_space=pltpu.VMEM)
    sems = []
    for count in (2, 2, members - 1, members // 2, members // 2, 3):
        sems += [pltpu.SemaphoreType.DMA((count,))] * 2

    def body(*refs):
        reduce_kernel(members, total, *refs)

    done, decs = pl.pallas_call(
        body,
        out_shape=[
            jax.ShapeDtypeStruct((grad_rows, width), F32),
            jax.ShapeDtypeStruct((quarters, dec_rows, width), F32),
        ],
        in_specs=[vmem],
        out_specs=[vmem] * 2,
        scratch_shapes=[
            pltpu.VMEM((2, grad_rows, width), F32),
            pltpu.VMEM((2 * width, width), BF16),
            pltpu.VMEM((tail_rows, width), F32),
            pltpu.VMEM((2 * width, width), BF16),
            pltpu.VMEM((tail_rows, width), F32),
            pltpu.VMEM((grad_rows, width), F32),
            pltpu.VMEM((members, piece, width), BF16),
            pltpu.VMEM((members - 1, piece, width), BF16),
        ]
        + sems,
        compiler_params=pltpu.CompilerParams(
            collective_id=1, has_side_effects=True, vmem_limit_bytes=60 * 1024 * 1024
        ),
        name="reduce_grads",
    )(grads)

    def finish(*refs):
        finish_kernel(rows, *refs)

    return pl.pallas_call(
        finish,
        out_shape=[
            jax.ShapeDtypeStruct((width, width), F32),
            jax.ShapeDtypeStruct((width, width), F32),
            jax.ShapeDtypeStruct((1, width), F32),
            jax.ShapeDtypeStruct((1, width), F32),
            jax.ShapeDtypeStruct((width, seen_width), F32),
            jax.ShapeDtypeStruct((1, 2), F32),
        ],
        in_specs=[vmem] * 2,
        out_specs=[vmem] * 6,
        compiler_params=pltpu.CompilerParams(vmem_limit_bytes=8 * 1024 * 1024),
        name="finish",
    )(done, decs)


def on_device(
    init_state,
    brownian,
    step_size,
    lengths,
    obs_steps,
    observed,
    w_in,
    b_in,
    w_out,
    b_out,
    decoder,
    prior_rate,
    diffusion,
):
    rows, width = init_state.shape
    seen_width = decoder.shape[1]
    w_in_all, w_out_all, b_in_all = gather(w_in, w_out, b_in[None, :])
    unit = 8 * lax.axis_size("batch")
    need = 2 * width + width // lax.axis_size("mp") * seen_width // width + 3
    elbo, grads, cot = core(
        -(-need // unit) * unit,
        init_state,
        brownian,
        step_size[None, :],
        lengths[None, :],
        obs_steps.T,
        observed,
        w_in_all,
        b_in_all,
        w_out_all,
        b_out[None, :],
        decoder,
        prior_rate[None, :],
        diffusion[None, :],
    )
    own_w_in, own_w_out, own_b_in, b_out_grad, dec_grad, scores = reduce_all(
        grads, rows, seen_width
    )
    return (
        elbo[0],
        scores[0],
        own_w_in,
        own_b_in[0],
        own_w_out,
        b_out_grad[0],
        dec_grad,
        cot,
    )


def solution(mesh):
    both = ("batch", "mp")
    placed = (
        P(both, None),
        P(None, both, None),
        P(both),
        P(both),
        P(both, None),
        P(both, None, None),
        P(None, "mp"),
        P("mp"),
        P("mp", None),
        P(),
        P(),
        P(),
        P(),
    )
    return jax.shard_map(
        on_device,
        mesh=mesh,
        in_specs=placed,
        out_specs=(
            P(both),
            P(),
            P(None, "mp"),
            P("mp"),
            P("mp", None),
            P(),
            P(),
            P(both, None),
        ),
        check_vma=False,
    )
```
